32 devices in a mesh: leaf: 8 (over z, y), sub: 4 (over x, core).
Axes of the slice: x: 2, y: 2, z: 4, core: 2. Of those that a mesh axis runs over, the one named last changes fastest.
Arguments:
- vectors: bfloat16 [64, 8192], P('sub', 'leaf'), may hold values from -6 to 6
- near_blocks: bfloat16 [32, 9, 256, 256], P(('leaf', 'sub')), may hold values from -0.125 to 0.125
- near_cols: int32 [32, 9], P(('leaf', 'sub')), may hold values from 0 to 31, as said below
- near_mask: int32 [32, 9], P(('leaf', 'sub')), may hold values from 0 to 1, as said below
- leaf_basis: bfloat16 [32, 32, 256], P('leaf'), may hold values from -0.375 to 0.375
- transfer: bfloat16 [48, 32, 32], P('leaf'), may hold values from -1 to 1
- coupling: bfloat16 [56, 27, 32, 32], P('leaf'), may hold values from -0.3125 to 0.3125
- far_targets: int32 [56, 27], P('leaf'), may hold values from 0 to 55, as said below
- far_mask: int32 [56, 27], P('leaf'), may hold values from 0 to 1
Outputs:
- result: bfloat16 [64, 8192], P('sub', 'leaf')
The draws below stay inside these ranges and needn't reach their ends.
Inputs may be any that keep to these rules, and one draw needn't show every extreme that they name: `near_cols`: row i names 9 leaves; its first entry is leaf i; every entry is a leaf of the subtree of leaf i or of the subtree just before or after it; the entries marked live are distinct. `near_mask`: the first entry of each row is 1. `far_targets`: entry (c, k) names a cluster on the same level as cluster c, in any subtree. The 189 entries of one subtree's rows, masked ones included, name clusters of any one subtree at most 32 times; in every draw some subtree is named exactly 32 times, by live entries, from every subtree.
All inputs are finite; a program needn't handle non-finite values.
Results may differ from the reference program's by a relative error of at most 0.0065.
Values may be sent and summed in bfloat16 or wider, within the bound.
No kernel may reach another device: no remote copies, remote signals or barrier semaphores. Data moves between devices by JAX's collectives and lax.ppermute only.
A program may use at most 64 MiB of HBM per device.

```python
import jax
import jax.numpy as jnp
from jax import lax

LEAF = 256
RANK = 32
VECS = 64
NEAR = 9
FAR = 27
SUBTREE = 4
CLUSTERS = 7
LEAVES = 32
POINTS = 8192
NODES = 56
SPAN = 8
CAP = 32
N_LEAF = 8


def near_lists(key):
    leaf_ids = jnp.arange(LEAVES, dtype=jnp.int32)
    width_all = 3 * SUBTREE
    position = jnp.arange(width_all, dtype=jnp.int32)
    scores = jax.random.randint(jax.random.fold_in(key, 11), (LEAVES, width_all), 0, 65536, dtype=jnp.int32)
    scores = scores * width_all + position[None, :]
    own_place = leaf_ids % SUBTREE + SUBTREE
    scores = jnp.where(position[None, :] == own_place[:, None], -1, scores)
    best_scores, chosen = lax.top_k(scores, NEAR - 1)
    window_first = (leaf_ids // SUBTREE - 1) * SUBTREE
    columns = window_first[:, None] + chosen.astype(jnp.int32)
    inside = (columns >= 0) & (columns < LEAVES)
    density = jax.random.randint(jax.random.fold_in(key, 12), (LEAVES, 1), 1, 5, dtype=jnp.int32)
    alive = (jax.random.randint(jax.random.fold_in(key, 13), (LEAVES, NEAR - 1), 0, 4, dtype=jnp.int32) < density) & inside
    columns = jnp.where(inside, columns, leaf_ids[:, None])
    columns = jnp.concatenate([leaf_ids[:, None], columns], axis=1).astype(jnp.int32)
    alive = jnp.concatenate([jnp.ones((LEAVES, 1), jnp.int32), alive.astype(jnp.int32)], axis=1)
    return (columns, alive)


def far_lists(key):
    pairs = CLUSTERS * FAR
    slots = SPAN * CAP
    half_span = SPAN // 2
    busiest = jax.random.randint(jax.random.fold_in(key, 21), (), 0, N_LEAF, dtype=jnp.int32)
    tree_ids = jnp.arange(N_LEAF, dtype=jnp.int32)
    slot_ids = jnp.arange(slots, dtype=jnp.int32)
    scores = jax.random.randint(jax.random.fold_in(key, 22), (N_LEAF, slots), 0, 65536, dtype=jnp.int32)
    scores = scores * slots + slot_ids[None, :]
    busy_offset = (busiest - tree_ids + half_span) % N_LEAF
    forced = slot_ids[None, :] // CAP == busy_offset[:, None]
    scores = jnp.where(forced, scores + 1073741824, scores)
    best_scores, chosen = lax.top_k(scores, pairs)
    order_keys = jax.random.split(jax.random.fold_in(key, 23), N_LEAF)
    orders = jax.vmap(lambda single: jax.random.permutation(single, pairs))(order_keys)
    assigned = jnp.take_along_axis(chosen.astype(jnp.int32), orders.astype(jnp.int32), axis=1)
    owners = (tree_ids[:, None] + assigned // CAP - half_span) % N_LEAF
    source_local = jnp.arange(pairs, dtype=jnp.int32) // FAR
    level_first = jnp.zeros((pairs,), jnp.int32)
    level_width = jnp.ones((pairs,), jnp.int32)
    level_start = 0
    level_size = SUBTREE
    while level_size >= 1:
        within = (source_local >= level_start) & (source_local < level_start + level_size)
        level_first = jnp.where(within, level_start, level_first)
        level_width = jnp.where(within, level_size, level_width)
        level_start = level_start + level_size
        level_size = level_size // 2
    picked = jax.random.randint(jax.random.fold_in(key, 24), (N_LEAF, pairs), 0, 1048576, dtype=jnp.int32) % level_width[None, :]
    targets = owners * CLUSTERS + level_first[None, :] + picked
    alive = (jax.random.randint(jax.random.fold_in(key, 25), (N_LEAF, pairs), 0, 4, dtype=jnp.int32) < 3) | (owners == busiest)
    return (targets.reshape(NODES, FAR).astype(jnp.int32), alive.astype(jnp.int32).reshape(NODES, FAR))


def draw_near_cols(key, part):
    return near_lists(key)[0]


def draw_near_mask(key, part):
    return near_lists(key)[1]


def draw_far_targets(key, part):
    return far_lists(key)[0]


def draw_far_mask(key, part):
    return far_lists(key)[1]


def levels(key, extent, shards, least, high):
    gain = 1.0
    for axis_at, parts in shards:
        steps = jax.random.uniform(jax.random.fold_in(jax.random.fold_in(key, 6), axis_at), (parts,), jnp.float32, least / len(shards), high / len(shards))
        gain = gain * jnp.repeat(jnp.exp(steps), extent[axis_at] // parts).reshape((-1,) + (1,) * (len(extent) - 1 - axis_at))
    return gain


def centred(key, shape, deviation, bound, cuts=(), kind=jnp.bfloat16):
    entries = jax.random.normal(key, shape, jnp.float32) * deviation
    if len(cuts) > 0:
        entries = levels(key, shape, cuts, -0.22, 0.18) * entries
    return jnp.clip(entries, min=-bound, max=bound).astype(kind)


def setup_inputs(seed: int = 0) -> dict:
    key_list = jax.random.split(jax.random.key(seed), 10)
    return {
        "vectors": centred(key_list[0], (VECS, POINTS), 1.0, 6.0, ((0, 4), (1, 8))),
        "near_blocks": centred(key_list[1], (LEAVES, NEAR, LEAF, LEAF), (LEAF * NEAR) ** -0.5, 0.125, ((0, 32),)),
        "near_cols": draw_near_cols(jax.random.fold_in(key_list[9], 71), 0),
        "near_mask": draw_near_mask(jax.random.fold_in(key_list[9], 71), 0),
        "leaf_basis": centred(key_list[4], (LEAVES, RANK, LEAF), LEAF ** -0.5, 0.375, ((0, 8),)),
        "transfer": centred(key_list[5], (N_LEAF * (CLUSTERS - 1), RANK, RANK), RANK ** -0.5, 1.0, ((0, 8),)),
        "coupling": centred(key_list[6], (NODES, FAR, RANK, RANK), (RANK * FAR // 2) ** -0.5, 0.3125, ((0, 8),)),
        "far_targets": draw_far_targets(jax.random.fold_in(key_list[9], 71), 0),
        "far_mask": draw_far_mask(jax.random.fold_in(key_list[9], 71), 0),
    }


def level_list():
    sizes_all = []
    level_size = SUBTREE
    while level_size >= 1:
        sizes_all.append(level_size)
        level_size = level_size // 2
    return sizes_all


def reference(vectors, near_blocks, near_cols, near_mask, leaf_basis, transfer, coupling, far_targets, far_mask):
    highest = lax.Precision.HIGHEST
    pieces = vectors.reshape(VECS, LEAVES, LEAF)

    def one_leaf(items):
        blocks, columns, alive = items
        taken = jnp.take(pieces, columns, axis=1).astype(jnp.float32)
        taken = taken * alive.astype(jnp.float32)[None, :, None]
        return jnp.einsum("vkp,kpq->vq", taken, blocks.astype(jnp.float32), precision=highest)

    near = lax.map(one_leaf, (near_blocks, near_cols, near_mask))
    near = jnp.transpose(near, (1, 0, 2)).reshape(VECS, POINTS)

    sizes_all = level_list()
    starts_all = [sum(sizes_all[:number]) for number in range(len(sizes_all))]
    coeffs = jnp.einsum("vnp,nrp->nvr", pieces.astype(jnp.float32), leaf_basis.astype(jnp.float32), precision=highest)
    coeffs = coeffs.reshape(N_LEAF, SUBTREE, VECS, RANK)
    maps_all = transfer.astype(jnp.float32).reshape(N_LEAF, CLUSTERS - 1, RANK, RANK)
    hats = [coeffs]
    for level_no in range(len(sizes_all) - 1):
        level_size = sizes_all[level_no]
        level_start = starts_all[level_no]
        child = hats[-1].reshape(N_LEAF, level_size // 2, 2, VECS, RANK)
        level_maps = maps_all[:, level_start:level_start + level_size].reshape(N_LEAF, level_size // 2, 2, RANK, RANK)
        hats.append(jnp.einsum("npcvr,npcrq->npvq", child, level_maps, precision=highest))
    all_hats = jnp.concatenate(hats, axis=1).reshape(NODES, VECS, RANK)
    terms = jnp.einsum("nvr,nkrq->nkvq", all_hats, coupling.astype(jnp.float32), precision=highest)
    terms = terms * far_mask.astype(jnp.float32)[:, :, None, None]
    incoming = jax.ops.segment_sum(terms.reshape(NODES * FAR, VECS, RANK), far_targets.reshape(-1), num_segments=NODES)
    incoming = incoming.reshape(N_LEAF, CLUSTERS, VECS, RANK)
    downward = [incoming[:, starts_all[number]:starts_all[number] + sizes_all[number]] for number in range(len(sizes_all))]
    for level_no in range(len(sizes_all) - 2, -1, -1):
        level_size = sizes_all[level_no]
        level_start = starts_all[level_no]
        level_maps = maps_all[:, level_start:level_start + level_size].reshape(N_LEAF, level_size // 2, 2, RANK, RANK)
        pushed = jnp.einsum("npvq,npcrq->npcvr", downward[level_no + 1], level_maps, precision=highest)
        downward[level_no] = downward[level_no] + pushed.reshape(N_LEAF, level_size, VECS, RANK)
    basis_tree = leaf_basis.astype(jnp.float32).reshape(N_LEAF, SUBTREE, RANK, LEAF)
    far = jnp.einsum("nsvr,nsrp->vnsp", downward[0], basis_tree, precision=highest).reshape(VECS, POINTS)
    return (near + far).astype(jnp.bfloat16)
```

```python
import functools

import jax
import jax.numpy as jnp
from jax import lax
from jax.experimental import pallas as pl
from jax.experimental.pallas import tpu as pltpu
from jax.sharding import PartitionSpec as P

LANES = 128


def flip(values, axis, bit):
    count = lax.axis_size(axis)
    return lax.ppermute(values, axis, [(i, i ^ bit) for i in range(count)])


def beside(values, axis):
    count = lax.axis_size(axis)
    other = [((i + 1) ^ 1) - 1 for i in range(count)]
    return lax.ppermute(
        values, axis, [(i, j if 0 <= j < count else i) for i, j in enumerate(other)]
    )


def levels_of(subtree):
    sizes = []
    while subtree >= 1:
        sizes.append(subtree)
        subtree = subtree // 2
    starts = [sum(sizes[:number]) for number in range(len(sizes))]
    return sizes, starts


def split_dot(left, right, contract):
    high = left.astype(jnp.bfloat16)
    low = (left - high.astype(jnp.float32)).astype(jnp.bfloat16)
    dims = (contract, ((), ()))
    return lax.dot_general(
        high, right, dims, preferred_element_type=jnp.float32
    ) + lax.dot_general(low, right, dims, preferred_element_type=jnp.float32)


def expand_kernel(
    leaf_count, targets, alive, vectors, basis, transfer, coupling, keep, send, *sums
):
    subtree, rank, leaf_size = basis.shape
    clusters, far_count = coupling.shape[:2]
    nodes = leaf_count * clusters
    sizes, starts = levels_of(subtree)
    rows = vectors.shape[0]
    parity = lax.axis_index("leaf") % 2
    hats = []
    for j in range(subtree):
        hats.append(
            lax.dot_general(
                vectors[:, j * leaf_size : (j + 1) * leaf_size],
                basis[j],
                (((1,), (1,)), ((), ())),
                preferred_element_type=jnp.float32,
            )
        )
    for number in range(len(sizes) - 1):
        for p in range(sizes[number + 1]):
            c = starts[number] + 2 * p
            hats.append(
                split_dot(hats[c], transfer[c], ((1,), (0,)))
                + split_dot(hats[c + 1], transfer[c + 1], ((1,), (0,)))
            )
    shared = len(sums) < clusters
    zero = jnp.zeros((rows, rank), jnp.float32)
    if shared:

        def clear(row, carry):
            sums[0][row] = zero
            return carry

        lax.fori_loop(0, nodes, clear, 0)
    else:
        for number, size in enumerate(sizes):
            for c in range(starts[number], starts[number] + size):
                for tree in range(leaf_count):
                    for j in range(starts[number], starts[number] + size):
                        sums[c][tree * clusters + j] = zero
    lefts = [hat.astype(jnp.bfloat16) for hat in hats]
    for k in range(far_count):
        for c in range(clusters):
            term = jnp.dot(lefts[c], coupling[c, k], preferred_element_type=jnp.float32)
            row = jnp.where(alive[c, k] == 1, targets[c, k], nodes)
            held = sums[0 if shared else c]
            held[row] = held[row] + term
    per = LANES // rank

    def gathered(tree):
        groups = []
        for first in range(0, clusters, per):
            lanes = []
            for place in range(first, first + per):
                if place >= clusters:
                    lanes.append(zero)
                    continue
                number = max(n for n in range(len(sizes)) if starts[n] <= place)
                row = tree * clusters + place
                if shared:
                    lanes.append(sums[0][row])
                else:
                    level = range(starts[number], starts[number] + sizes[number])
                    lanes.append(sum(sums[c][row] for c in level))
            groups.append(jnp.concatenate(lanes, axis=1))
        return groups

    def emit(half, carry):
        for out, tree in ((keep, 2 * half + parity), (send, 2 * half + 1 - parity)):
            for number, group in enumerate(gathered(tree)):
                out[half, number] = group.astype(out.dtype)
        return carry

    if leaf_count <= 8:
        for half in range(leaf_count // 2):
            emit(half, 0)
    else:
        lax.fori_loop(0, leaf_count // 2, emit, 0)


def expand(vectors, basis, transfer, coupling, targets, alive):
    leaf_count = lax.axis_size("leaf")
    clusters, far_count, rank = coupling.shape[:3]
    rows = vectors.shape[0]
    nodes = leaf_count * clusters
    groups = -(-clusters * rank // LANES)
    shape = (leaf_count // 2, groups, rows, LANES)
    copies = clusters if nodes <= 128 else 1
    smem = pl.BlockSpec(memory_space=pltpu.SMEM)
    vmem = pl.BlockSpec(memory_space=pltpu.VMEM)
    return pl.pallas_call(
        functools.partial(expand_kernel, leaf_count),
        out_shape=[
            jax.ShapeDtypeStruct(shape, jnp.float32),
            jax.ShapeDtypeStruct(shape, jnp.bfloat16),
        ],
        in_specs=[smem, smem, vmem, vmem, vmem, vmem],
        out_specs=[vmem, vmem],
        scratch_shapes=[pltpu.VMEM((nodes + 1, rows, rank), jnp.float32)] * copies,
        name="expand",
    )(targets, alive, vectors, basis, transfer, coupling)


def near_kernel(
    sub_count, columns, alive, blocks, *refs
):
    pieces, (own, *outs), window = refs[: len(refs) - sub_count - 1], refs[-sub_count - 1 : -1], refs[-1]
    per_tree = len(pieces) // 3
    rows, points = pieces[0].shape
    count, leaf_size = blocks.shape[1:3]
    subtree = points // leaf_size
    for tree in range(3):
        for part in range(per_tree):
            window[tree, part * rows : (part + 1) * rows, :] = pieces[tree * per_tree + part][...]
    me = lax.axis_index("leaf")
    first = me * subtree
    partner = (me ^ 1) * subtree
    total = None
    for k in range(count):
        column = columns[0, k]
        own_tree = (column >= first) & (column < first + subtree)
        partner_tree = (column >= partner) & (column < partner + subtree)
        tree = jnp.where(own_tree, 0, jnp.where(partner_tree, 1, 2))
        place = lax.rem(column, subtree)
        start = pl.multiple_of(place * leaf_size, leaf_size)
        taken = window[tree, :, pl.ds(start, leaf_size)]
        live = alive[0, k].astype(jnp.float32).astype(jnp.bfloat16)
        product = jnp.dot(taken * live, blocks[0, k], preferred_element_type=jnp.float32)
        total = product if total is None else total + product
    size = total.shape[0] // sub_count
    for number, out in enumerate((own, *outs)):
        out[...] = total[number * size : (number + 1) * size].astype(out.dtype)


def near(pieces, blocks, columns, alive, rows):
    sub_count = lax.axis_size("sub")
    leaf_size = blocks.shape[2]
    smem = pl.BlockSpec(memory_space=pltpu.SMEM)
    vmem = pl.BlockSpec(memory_space=pltpu.VMEM)
    points = pieces[0].shape[1]
    return pl.pallas_call(
        functools.partial(near_kernel, sub_count),
        out_shape=[jax.ShapeDtypeStruct((rows, leaf_size), jnp.float32)]
        + [jax.ShapeDtypeStruct((rows, leaf_size), jnp.bfloat16)] * (sub_count - 1),
        in_specs=[smem, smem] + [vmem] * (1 + len(pieces)),
        out_specs=[vmem] * sub_count,
        scratch_shapes=[pltpu.VMEM((3, rows * sub_count, points), jnp.bfloat16)],
        name="near",
    )(columns, alive, blocks, *pieces)


def finish_kernel(keep, got, transfer, basis, *refs):
    subtree, rank, leaf_size = basis.shape
    nears, out = refs[:-1], refs[-1]
    sizes, starts = levels_of(subtree)
    clusters = sum(sizes)
    per = LANES // rank
    incoming = [keep[0, g] + got[0, g].astype(jnp.float32) for g in range(keep.shape[1])]
    down = [
        incoming[c // per][:, (c % per) * rank : (c % per + 1) * rank] for c in range(clusters)
    ]
    for number in range(len(sizes) - 2, -1, -1):
        for j in range(sizes[number]):
            c = starts[number] + j
            parent = starts[number + 1] + j // 2
            down[c] = down[c] + split_dot(down[parent], transfer[c], ((1,), (1,)))
    me = lax.axis_index("sub")
    for j in range(subtree):
        columns = slice(j * leaf_size, (j + 1) * leaf_size)
        out[:, columns] = jnp.zeros((out.shape[0], leaf_size), out.dtype)
    far = [split_dot(down[j], basis[j], ((1,), (0,))) for j in range(subtree)]
    for j in range(subtree):
        piece = nears[0][...]
        for other in range(1, subtree):
            piece = jnp.where((me ^ other) == j, nears[other][...].astype(jnp.float32), piece)
        out[:, j * leaf_size : (j + 1) * leaf_size] = (piece + far[j]).astype(out.dtype)


def finish(keep, got, transfer, basis, nears):
    rows = nears[0].shape[0]
    subtree, _, leaf_size = basis.shape
    vmem = pl.BlockSpec(memory_space=pltpu.VMEM)
    return pl.pallas_call(
        finish_kernel,
        out_shape=jax.ShapeDtypeStruct((rows, subtree * leaf_size), jnp.bfloat16),
        in_specs=[vmem] * (4 + len(nears)),
        out_specs=vmem,
        name="finish",
    )(keep, got, transfer, basis, *nears)


def local(
    vectors,
    near_blocks,
    near_cols,
    near_mask,
    leaf_basis,
    transfer,
    coupling,
    far_targets,
    far_mask,
):
    leaf_count = lax.axis_size("leaf")
    sub_count = lax.axis_size("sub")
    me = lax.axis_index("leaf")
    rows = vectors.shape[0]
    half = sub_count // 2
    pair = jnp.concatenate([vectors, flip(vectors, "sub", half)], axis=0)
    keep, send = expand(vectors, leaf_basis, transfer, coupling, far_targets, far_mask)
    got = flip(send, "leaf", 1)
    trees = [[pair], [flip(pair, "leaf", 1)], [beside(pair, "leaf")]]
    order = [0, half]
    bit = half // 2
    while bit >= 1:
        trees = [parts + [flip(part, "sub", bit) for part in parts] for parts in trees]
        order = order + [number ^ bit for number in order]
        bit = bit // 2
    pieces = [part for parts in trees for part in parts]
    size = leaf_count // 2
    while size > 1:
        total = (keep + got.astype(keep.dtype)).reshape(2, size // 2, *keep.shape[1:])
        mine = (me // size) % 2
        keep = lax.dynamic_index_in_dim(total, mine, 0, keepdims=False)
        send = lax.dynamic_index_in_dim(total, 1 - mine, 0, keepdims=False)
        got = flip(send.astype(jnp.bfloat16), "leaf", size)
        size = size // 2
    made = near(pieces, near_blocks, near_cols, near_mask, rows)
    nears = [None] * sub_count
    for number, away in zip(order, made):
        nears[number] = away if number == 0 else flip(away, "sub", number)
    return finish(keep, got, transfer, leaf_basis, nears)


def solution(mesh):
    return jax.shard_map(
        local,
        mesh=mesh,
        in_specs=(
            P("sub", "leaf"),
            P(("leaf", "sub"), None, None, None),
            P(("leaf", "sub"), None),
            P(("leaf", "sub"), None),
            P("leaf", None, None),
            P("leaf", None, None),
            P("leaf", None, None, None),
            P("leaf", None),
            P("leaf", None),
        ),
        out_specs=P("sub", "leaf"),
        check_vma=False,
    )
```

```python
import functools

import jax
import jax.numpy as jnp
from jax import lax
from jax.experimental import pallas as pl
from jax.experimental.pallas import tpu as pltpu
from jax.sharding import PartitionSpec as P

LANES = 128
PARAMS = pltpu.CompilerParams(vmem_limit_bytes=16 * 2**20)


def flip(values, axis, bit):
    count = lax.axis_size(axis)
    return lax.ppermute(values, axis, [(i, i ^ bit) for i in range(count)])


def beside(values, axis):
    count = lax.axis_size(axis)
    other = [((i + 1) ^ 1) - 1 for i in range(count)]
    return lax.ppermute(
        values, axis, [(i, j if 0 <= j < count else i) for i, j in enumerate(other)]
    )


def levels_of(subtree):
    sizes = []
    while subtree >= 1:
        sizes.append(subtree)
        subtree = subtree // 2
    starts = [sum(sizes[:number]) for number in range(len(sizes))]
    return sizes, starts


def split_dot(left, right, contract):
    high = left.astype(jnp.bfloat16)
    low = (left - high.astype(jnp.float32)).astype(jnp.bfloat16)
    dims = (contract, ((), ()))
    return lax.dot_general(
        high, right, dims, preferred_element_type=jnp.float32
    ) + lax.dot_general(low, right, dims, preferred_element_type=jnp.float32)


def expand_kernel(
    leaf_count, targets, alive, vectors, basis, transfer, coupling, keep, send, *sums
):
    subtree, rank, leaf_size = basis.shape
    clusters, far_count = coupling.shape[:2]
    nodes = leaf_count * clusters
    sizes, starts = levels_of(subtree)
    rows = vectors.shape[0]
    parity = lax.axis_index("leaf") % 2
    hats = []
    for j in range(subtree):
        hats.append(
            lax.dot_general(
                vectors[:, j * leaf_size : (j + 1) * leaf_size],
                basis[j],
                (((1,), (1,)), ((), ())),
                preferred_element_type=jnp.float32,
            )
        )
    for number in range(len(sizes) - 1):
        for p in range(sizes[number + 1]):
            c = starts[number] + 2 * p
            hats.append(
                split_dot(hats[c], transfer[c], ((1,), (0,)))
                + split_dot(hats[c + 1], transfer[c + 1], ((1,), (0,)))
            )
    shared = len(sums) < clusters
    zero = jnp.zeros((rows, rank), jnp.float32)
    if shared:

        def clear(row, carry):
            sums[0][row] = zero
            return carry

        lax.fori_loop(0, nodes, clear, 0)
    else:
        for number, size in enumerate(sizes):
            for c in range(starts[number], starts[number] + size):
                for tree in range(leaf_count):
                    for j in range(starts[number], starts[number] + size):
                        sums[c][tree * clusters + j] = zero
    lefts = [hat.astype(jnp.bfloat16) for hat in hats]
    for k in range(far_count):
        for c in range(clusters):
            term = jnp.dot(lefts[c], coupling[c, k], preferred_element_type=jnp.float32)
            row = jnp.where(alive[c, k] == 1, targets[c, k], nodes)
            held = sums[0 if shared else c]
            held[row] = held[row] + term
    per = LANES // rank

    def gathered(tree):
        groups = []
        for first in range(0, clusters, per):
            lanes = []
            for place in range(first, first + per):
                if place >= clusters:
                    lanes.append(zero)
                    continue
                number = max(n for n in range(len(sizes)) if starts[n] <= place)
                row = tree * clusters + place
                if shared:
                    lanes.append(sums[0][row])
                else:
                    level = range(starts[number], starts[number] + sizes[number])
                    lanes.append(sum(sums[c][row] for c in level))
            groups.append(jnp.concatenate(lanes, axis=1))
        return groups

    def emit(half, carry):
        for out, tree in ((keep, 2 * half + parity), (send, 2 * half + 1 - parity)):
            for number, group in enumerate(gathered(tree)):
                out[half, number] = group.astype(out.dtype)
        return carry

    if leaf_count <= 8:
        for half in range(leaf_count // 2):
            emit(half, 0)
    else:
        lax.fori_loop(0, leaf_count // 2, emit, 0)


def expand(vectors, basis, transfer, coupling, targets, alive):
    leaf_count = lax.axis_size("leaf")
    clusters, far_count, rank = coupling.shape[:3]
    rows = vectors.shape[0]
    nodes = leaf_count * clusters
    groups = -(-clusters * rank // LANES)
    shape = (leaf_count // 2, groups, rows, LANES)
    copies = clusters if nodes <= 128 else 1
    smem = pl.BlockSpec(memory_space=pltpu.SMEM)
    vmem = pl.BlockSpec(memory_space=pltpu.VMEM)
    return pl.pallas_call(
        functools.partial(expand_kernel, leaf_count),
        out_shape=[
            jax.ShapeDtypeStruct(shape, jnp.float32),
            jax.ShapeDtypeStruct(shape, jnp.bfloat16),
        ],
        in_specs=[smem, smem, vmem, vmem, vmem, vmem],
        out_specs=[vmem, vmem],
        scratch_shapes=[pltpu.VMEM((nodes + 1, rows, rank), jnp.float32)] * copies,
        compiler_params=PARAMS,
        name="expand",
    )(targets, alive, vectors, basis, transfer, coupling)


def near_kernel(
    sub_count, columns, alive, blocks, *refs
):
    pieces, (own, *outs), window = refs[: len(refs) - sub_count - 1], refs[-sub_count - 1 : -1], refs[-1]
    per_tree = len(pieces) // 3
    rows, points = pieces[0].shape
    count, leaf_size = blocks.shape[1:3]
    subtree = points // leaf_size
    for tree in range(3):
        for part in range(per_tree):
            window[tree, part * rows : (part + 1) * rows, :] = pieces[tree * per_tree + part][...]
    me = lax.axis_index("leaf")
    first = me * subtree
    partner = (me ^ 1) * subtree
    total = None
    for k in range(count):
        column = columns[0, k]
        own_tree = (column >= first) & (column < first + subtree)
        partner_tree = (column >= partner) & (column < partner + subtree)
        tree = jnp.where(own_tree, 0, jnp.where(partner_tree, 1, 2))
        place = lax.rem(column, subtree)
        start = pl.multiple_of(place * leaf_size, leaf_size)
        taken = window[tree, :, pl.ds(start, leaf_size)]
        live = alive[0, k].astype(jnp.float32).astype(jnp.bfloat16)
        product = jnp.dot(taken * live, blocks[0, k], preferred_element_type=jnp.float32)
        total = product if total is None else total + product
    size = total.shape[0] // sub_count
    for number, out in enumerate((own, *outs)):
        out[...] = total[number * size : (number + 1) * size].astype(out.dtype)


def near(pieces, blocks, columns, alive, rows):
    sub_count = lax.axis_size("sub")
    leaf_size = blocks.shape[2]
    smem = pl.BlockSpec(memory_space=pltpu.SMEM)
    vmem = pl.BlockSpec(memory_space=pltpu.VMEM)
    points = pieces[0].shape[1]
    return pl.pallas_call(
        functools.partial(near_kernel, sub_count),
        out_shape=[jax.ShapeDtypeStruct((rows, leaf_size), jnp.float32)]
        + [jax.ShapeDtypeStruct((rows, leaf_size), jnp.bfloat16)] * (sub_count - 1),
        in_specs=[smem, smem] + [vmem] * (1 + len(pieces)),
        out_specs=[vmem] * sub_count,
        scratch_shapes=[pltpu.VMEM((3, rows * sub_count, points), jnp.bfloat16)],
        compiler_params=PARAMS,
        name="near",
    )(columns, alive, blocks, *pieces)


def finish_kernel(keep, got, transfer, basis, *refs):
    subtree, rank, leaf_size = basis.shape
    nears, out = refs[:-1], refs[-1]
    sizes, starts = levels_of(subtree)
    clusters = sum(sizes)
    per = LANES // rank
    incoming = [keep[0, g] + got[0, g].astype(jnp.float32) for g in range(keep.shape[1])]
    down = [
        incoming[c // per][:, (c % per) * rank : (c % per + 1) * rank] for c in range(clusters)
    ]
    for number in range(len(sizes) - 2, -1, -1):
        for j in range(sizes[number]):
            c = starts[number] + j
            parent = starts[number + 1] + j // 2
            down[c] = down[c] + split_dot(down[parent], transfer[c], ((1,), (1,)))
    me = lax.axis_index("sub")
    for j in range(subtree):
        columns = slice(j * leaf_size, (j + 1) * leaf_size)
        out[:, columns] = jnp.zeros((out.shape[0], leaf_size), out.dtype)
    far = [split_dot(down[j], basis[j], ((1,), (0,))) for j in range(subtree)]
    for j in range(subtree):
        piece = nears[0][...]
        for other in range(1, subtree):
            piece = jnp.where((me ^ other) == j, nears[other][...].astype(jnp.float32), piece)
        out[:, j * leaf_size : (j + 1) * leaf_size] = (piece + far[j]).astype(out.dtype)


def finish(keep, got, transfer, basis, nears):
    rows = nears[0].shape[0]
    subtree, _, leaf_size = basis.shape
    vmem = pl.BlockSpec(memory_space=pltpu.VMEM)
    return pl.pallas_call(
        finish_kernel,
        out_shape=jax.ShapeDtypeStruct((rows, subtree * leaf_size), jnp.bfloat16),
        in_specs=[vmem] * (4 + len(nears)),
        out_specs=vmem,
        compiler_params=PARAMS,
        name="finish",
    )(keep, got, transfer, basis, *nears)


def local(
    vectors,
    near_blocks,
    near_cols,
    near_mask,
    leaf_basis,
    transfer,
    coupling,
    far_targets,
    far_mask,
):
    leaf_count = lax.axis_size("leaf")
    sub_count = lax.axis_size("sub")
    me = lax.axis_index("leaf")
    rows = vectors.shape[0]
    half = sub_count // 2
    pair = jnp.concatenate([vectors, flip(vectors, "sub", half)], axis=0)
    keep, send = expand(vectors, leaf_basis, transfer, coupling, far_targets, far_mask)
    got = flip(send, "leaf", 1)
    trees = [[pair], [flip(pair, "leaf", 1)], [beside(pair, "leaf")]]
    order = [0, half]
    bit = half // 2
    while bit >= 1:
        trees = [parts + [flip(part, "sub", bit) for part in parts] for parts in trees]
        order = order + [number ^ bit for number in order]
        bit = bit // 2
    pieces = [part for parts in trees for part in parts]
    size = leaf_count // 2
    while size > 1:
        total = (keep + got.astype(keep.dtype)).reshape(2, size // 2, *keep.shape[1:])
        mine = (me // size) % 2
        keep = lax.dynamic_index_in_dim(total, mine, 0, keepdims=False)
        send = lax.dynamic_index_in_dim(total, 1 - mine, 0, keepdims=False)
        got = flip(send.astype(jnp.bfloat16), "leaf", size)
        size = size // 2
    made = near(pieces, near_blocks, near_cols, near_mask, rows)
    nears = [None] * sub_count
    for number, away in zip(order, made):
        nears[number] = away if number == 0 else flip(away, "sub", number)
    return finish(keep, got, transfer, leaf_basis, nears)


def solution(mesh):
    return jax.shard_map(
        local,
        mesh=mesh,
        in_specs=(
            P("sub", "leaf"),
            P(("leaf", "sub"), None, None, None),
            P(("leaf", "sub"), None),
            P(("leaf", "sub"), None),
            P("leaf", None, None),
            P("leaf", None, None),
            P("leaf", None, None, None),
            P("leaf", None),
            P("leaf", None),
        ),
        out_specs=P("sub", "leaf"),
        check_vma=False,
    )
```

```python
import functools

import jax
import jax.numpy as jnp
from jax import lax
from jax.experimental import pallas as pl
from jax.experimental.pallas import tpu as pltpu
from jax.sharding import PartitionSpec as P


LANES = 128
PARAMS = pltpu.CompilerParams(vmem_limit_bytes=16 * 2**20)
SMEM = pl.BlockSpec(memory_space=pltpu.SMEM)
VMEM = pl.BlockSpec(memory_space=pltpu.VMEM)
HBM = pl.BlockSpec(memory_space=pltpu.HBM)


def flip(values, axis, bit):
    count = lax.axis_size(axis)
    return lax.ppermute(values, axis, [(i, i ^ bit) for i in range(count)])


def beside(values, axis):
    count = lax.axis_size(axis)
    other = [((i + 1) ^ 1) - 1 for i in range(count)]
    pairs = [(i, j if 0 <= j < count else i) for i, j in enumerate(other)]
    return lax.ppermute(values, axis, pairs)


def bits_of(count):
    bits = []
    while count > 1:
        count = count // 2
        bits.append(count)
    return bits


def levels_of(subtree):
    sizes = []
    while subtree >= 1:
        sizes.append(subtree)
        subtree = subtree // 2
    starts = [sum(sizes[:number]) for number in range(len(sizes))]
    return sizes, starts


def halves(values):
    high = values.astype(jnp.bfloat16)
    return high, (values - high.astype(jnp.float32)).astype(jnp.bfloat16)


def dot(left, right, contract=((1,), (0,))):
    return lax.dot_general(left, right, (contract, ((), ())), preferred_element_type=jnp.float32)


def expand_kernel(
    leaf_count, targets_in, alive_in, vectors_in, basis_in, transfer_in, coupling_in, keep, send, *scratch
):
    targets, alive, vectors, basis, transfer, coupling, done, *sums = scratch
    subtree, rank, leaf_size = basis.shape
    clusters, far_count = coupling.shape[:2]
    nodes = leaf_count * clusters
    sizes, starts = levels_of(subtree)
    rows = vectors.shape[0]
    parity = lax.axis_index("leaf") % 2
    copies = [
        pltpu.make_async_copy(source, target, done.at[number])
        for number, (source, target) in enumerate(
            (
                (vectors_in, vectors),
                (basis_in, basis),
                (coupling_in.at[:subtree], coupling.at[:subtree]),
                (transfer_in, transfer),
                (targets_in, targets),
                (alive_in, alive),
                (coupling_in.at[subtree:], coupling.at[subtree:]),
            )
        )
    ]
    for copy in copies:
        copy.start()
    zero = jnp.zeros((rows, rank), jnp.float32)
    shared = len(sums) < clusters
    if shared:

        def clear(row, carry):
            sums[0][row] = zero
            return carry

        lax.fori_loop(0, nodes, clear, 0)
    else:
        for number, size in enumerate(sizes):
            for c in range(starts[number], starts[number] + size):
                for tree in range(leaf_count):
                    for j in range(starts[number], starts[number] + size):
                        sums[c][tree * clusters + j] = zero
    copies[0].wait()
    copies[1].wait()
    hats = [
        dot(vectors[:, j * leaf_size : (j + 1) * leaf_size], basis[j], ((1,), (1,)))
        for j in range(subtree)
    ]
    copies[3].wait()
    for number in range(len(sizes) - 1):
        for p in range(sizes[number + 1]):
            total = None
            for c in (starts[number] + 2 * p, starts[number] + 2 * p + 1):
                high, low = halves(hats[c])
                part = dot(high, transfer[c]) + dot(low, transfer[c])
                total = part if total is None else total + part
            hats.append(total)
    lefts = [hat.astype(jnp.bfloat16) for hat in hats]
    copies[4].wait()
    copies[5].wait()
    for wait, members in ((2, range(subtree)), (6, range(subtree, clusters))):
        copies[wait].wait()
        for k in range(far_count):
            for c in members:
                term = dot(lefts[c], coupling[c, k])
                row = jnp.where(alive[c, k] == 1, targets[c, k], nodes)
                held = sums[0 if shared else c]
                held[row] = held[row] + term
    per = LANES // rank

    def gathered(tree):
        groups = []
        for first in range(0, clusters, per):
            lanes = []
            for place in range(first, first + per):
                if place >= clusters:
                    lanes.append(zero)
                    continue
                number = max(n for n in range(len(sizes)) if starts[n] <= place)
                row = tree * clusters + place
                if shared:
                    lanes.append(sums[0][row])
                else:
                    level = range(starts[number], starts[number] + sizes[number])
                    lanes.append(sum(sums[c][row] for c in level))
            groups.append(jnp.concatenate(lanes, axis=1))
        return groups

    def emit(half, carry):
        for out, tree in ((keep, 2 * half + parity), (send, 2 * half + 1 - parity)):
            for number, group in enumerate(gathered(tree)):
                out[half, number] = group.astype(out.dtype)
        return carry

    if leaf_count <= 8:
        for half in range(leaf_count // 2):
            emit(half, 0)
    else:
        lax.fori_loop(0, leaf_count // 2, emit, 0)


def expand(vectors, basis, transfer, coupling, targets, alive):
    leaf_count = lax.axis_size("leaf")
    clusters, _, rank = coupling.shape[:3]
    rows = vectors.shape[0]
    nodes = leaf_count * clusters
    groups = -(-clusters * rank // LANES)
    shape = (leaf_count // 2, groups, rows, LANES)
    copies = clusters if nodes <= 128 else 1
    return pl.pallas_call(
        functools.partial(expand_kernel, leaf_count),
        out_shape=[
            jax.ShapeDtypeStruct(shape, jnp.float32),
            jax.ShapeDtypeStruct(shape, jnp.bfloat16),
        ],
        in_specs=[HBM] * 6,
        out_specs=[VMEM, VMEM],
        scratch_shapes=[
            pltpu.SMEM(targets.shape, targets.dtype),
            pltpu.SMEM(alive.shape, alive.dtype),
            pltpu.VMEM(vectors.shape, vectors.dtype),
            pltpu.VMEM(basis.shape, basis.dtype),
            pltpu.VMEM(transfer.shape, transfer.dtype),
            pltpu.VMEM(coupling.shape, coupling.dtype),
            pltpu.SemaphoreType.DMA((7,)),
        ]
        + [pltpu.VMEM((nodes + 1, rows, rank), jnp.float32)] * copies,
        compiler_params=PARAMS,
        name="expand",
    )(
        *(
            pltpu.with_memory_space_constraint(value, pltpu.HBM)
            for value in (targets, alive, vectors, basis, transfer, coupling)
        )
    )


def operator_kernel(transfer, basis, high_out, low_out):
    subtree, rank, leaf_size = basis.shape
    sizes, starts = levels_of(subtree)
    high_out[...] = jnp.zeros(high_out.shape, high_out.dtype)
    low_out[...] = jnp.zeros(low_out.shape, low_out.dtype)
    for j in range(subtree):
        columns = slice(j * leaf_size, (j + 1) * leaf_size)
        parts = (basis[j],)
        c = j
        for number in range(len(sizes)):
            at = slice(c * rank, (c + 1) * rank)
            high_out[at, columns] = parts[0]
            if len(parts) > 1:
                low_out[at, columns] = parts[1]
            if number + 1 < len(sizes):
                total = sum(dot(transfer[c], part, ((0,), (0,))) for part in parts)
                parts = halves(total)
                c = starts[number + 1] + (c - starts[number]) // 2


def operator(transfer, basis, depth):
    subtree, _, leaf_size = basis.shape
    shape = jax.ShapeDtypeStruct((depth, subtree * leaf_size), jnp.bfloat16)
    return pl.pallas_call(
        operator_kernel,
        out_shape=[shape, shape],
        in_specs=[VMEM, VMEM],
        out_specs=[VMEM, VMEM],
        compiler_params=PARAMS,
        name="operator",
    )(transfer, basis)


def near_kernel(places, sub_count, columns, alive, blocks, *refs):
    window, outs, pieces = refs[-1], refs[-1 - len(places) : -1], refs[: -1 - len(places)]
    per_tree = len(pieces) // 3
    rows, points = pieces[0].shape
    count, leaf_size = blocks.shape[1:3]
    subtree = points // leaf_size
    for tree in range(3):
        for part in range(per_tree):
            window[tree, part * rows : (part + 1) * rows, :] = pieces[tree * per_tree + part][...]
    me = lax.axis_index("leaf")
    first = me * subtree
    partner = (me ^ 1) * subtree
    total = None
    for k in range(count):
        column = columns[0, k]
        own_tree = (column >= first) & (column < first + subtree)
        partner_tree = (column >= partner) & (column < partner + subtree)
        tree = jnp.where(own_tree, 0, jnp.where(partner_tree, 1, 2))
        place = lax.rem(column, subtree)
        start = pl.multiple_of(place * leaf_size, leaf_size)
        taken = window[tree, :, pl.ds(start, leaf_size)]
        live = alive[0, k].astype(jnp.float32).astype(jnp.bfloat16)
        product = dot(taken * live, blocks[0, k])
        total = product if total is None else total + product
    size = total.shape[0] // sub_count
    for out, groups in zip(outs, places):
        for number, group in enumerate(groups):
            out[number] = total[group * size : (group + 1) * size].astype(out.dtype)


def near(pieces, blocks, columns, alive, rows, places):
    sub_count = lax.axis_size("sub")
    leaf_size = blocks.shape[2]
    points = pieces[0].shape[1]
    return pl.pallas_call(
        functools.partial(near_kernel, places, sub_count),
        out_shape=[
            jax.ShapeDtypeStruct(
                (len(groups), rows, leaf_size), jnp.bfloat16 if number else jnp.float32
            )
            for number, groups in enumerate(places)
        ],
        in_specs=[SMEM, SMEM] + [VMEM] * (1 + len(pieces)),
        out_specs=[VMEM] * len(places),
        scratch_shapes=[pltpu.VMEM((3, rows * sub_count, points), jnp.bfloat16)],
        compiler_params=PARAMS,
        name="near",
    )(columns, alive, blocks, *pieces)


def finish_kernel(sources, keep, got, high_in, low_in, *refs):
    nears, out = refs[:-1], refs[-1]
    incoming = jnp.concatenate(
        [keep[0, g] + got[0, g].astype(jnp.float32) for g in range(keep.shape[1])], axis=1
    )
    high, low = halves(incoming)
    far = dot(high, high_in[...]) + dot(low, high_in[...]) + dot(high, low_in[...])
    me = lax.axis_index("sub")
    leaf_size = nears[0].shape[2]
    pieces = [(source, nears[at][row].astype(jnp.float32)) for source, at, row in sources]
    for j in range(len(sources)):
        piece = pieces[0][1]
        for source, values in pieces[1:]:
            piece = jnp.where((me ^ source) == j, values, piece)
        columns = slice(j * leaf_size, (j + 1) * leaf_size)
        out[:, columns] = (piece + far[:, columns]).astype(out.dtype)


def finish(keep, got, high, low, nears, sources):
    rows = nears[0].shape[1]
    return pl.pallas_call(
        functools.partial(finish_kernel, sources),
        out_shape=jax.ShapeDtypeStruct((rows, high.shape[1]), jnp.bfloat16),
        in_specs=[VMEM] * (4 + len(nears)),
        out_specs=VMEM,
        compiler_params=PARAMS,
        name="finish",
    )(keep, got, high, low, *nears)


def local(
    vectors,
    near_blocks,
    near_cols,
    near_mask,
    leaf_basis,
    transfer,
    coupling,
    far_targets,
    far_mask,
):
    leaf_count = lax.axis_size("leaf")
    sub_count = lax.axis_size("sub")
    me = lax.axis_index("leaf")
    rows = vectors.shape[0]
    bits = bits_of(sub_count)
    pair = jnp.concatenate([vectors, flip(vectors, "sub", bits[0])], axis=0)
    keep, send = expand(vectors, leaf_basis, transfer, coupling, far_targets, far_mask)
    trees = [[pair], [flip(pair, "leaf", 1)], [beside(pair, "leaf")]]
    got = flip(send, "leaf", 1)
    order = [0, bits[0]]
    for bit in bits[1:]:
        trees = [parts + [flip(part, "sub", bit) for part in parts] for parts in trees]
        order = order + [number ^ bit for number in order]
    pieces = [part for parts in trees for part in parts]
    high, low = operator(transfer, leaf_basis, keep.shape[1] * LANES)
    for size in bits_of(leaf_count)[:-1]:
        total = (keep + got.astype(keep.dtype)).reshape(2, size // 2, *keep.shape[1:])
        mine = (me & size) // size
        keep = lax.dynamic_index_in_dim(total, mine, 0, keepdims=False)
        send = lax.dynamic_index_in_dim(total, 1 - mine, 0, keepdims=False)
        got = flip(send.astype(jnp.bfloat16), "leaf", size)
    places = [[order.index(0)]] + [
        [order.index(home) for home in range(bit, 2 * bit)] for bit in bits
    ]
    made = near(pieces, near_blocks, near_cols, near_mask, rows, places)
    arrays = list(made)
    pool = {0: [(0, 0, 0)]}
    for number, bit in enumerate(bits):
        for row in range(bit):
            pool[bit + row] = [(0, number + 1, row)]
    for bit in bits:
        sent = [(home, item) for home in range(bit, 2 * bit) for item in pool[home]]
        if len(sent) == arrays[sent[0][1][1]].shape[0]:
            stack = arrays[sent[0][1][1]]
        else:
            stack = jnp.concatenate([arrays[at][row : row + 1] for _, (_, at, row) in sent], axis=0)
        arrays.append(flip(stack, "sub", bit))
        for row, (home, (source, _, _)) in enumerate(sent):
            pool[home ^ bit].append((source ^ bit, len(arrays) - 1, row))
    used = sorted({at for _, at, _ in pool[0]})
    sources = [(source, used.index(at), row) for source, at, row in pool[0]]
    return finish(keep, got, high, low, [arrays[at] for at in used], sources)


def solution(mesh):
    return jax.shard_map(
        local,
        mesh=mesh,
        in_specs=(
            P("sub", "leaf"),
            P(("leaf", "sub"), None, None, None),
            P(("leaf", "sub"), None),
            P(("leaf", "sub"), None),
            P("leaf", None, None),
            P("leaf", None, None),
            P("leaf", None, None, None),
            P("leaf", None),
            P("leaf", None),
        ),
        out_specs=P("sub", "leaf"),
        check_vma=False,
    )
```

```python
import functools

import jax
import jax.numpy as jnp
from jax import lax
from jax.experimental import pallas as pl
from jax.experimental.pallas import tpu as pltpu
from jax.sharding import PartitionSpec as P


LANES = 128
PARAMS = pltpu.CompilerParams(vmem_limit_bytes=16 * 2**20)
SMEM = pl.BlockSpec(memory_space=pltpu.SMEM)
VMEM = pl.BlockSpec(memory_space=pltpu.VMEM)
HBM = pl.BlockSpec(memory_space=pltpu.HBM)


def flip(values, axis, bit):
    count = lax.axis_size(axis)
    return lax.ppermute(values, axis, [(i, i ^ bit) for i in range(count)])


def beside(values):
    leaf_count, sub_count = lax.axis_size("leaf"), lax.axis_size("sub")
    pairs = []
    for leaf in range(leaf_count):
        other = ((leaf + 1) ^ 1) - 1
        for sub in range(sub_count):
            here = leaf * sub_count + sub
            if 0 <= other < leaf_count:
                pairs.append((here, other * sub_count + sub))
            else:
                pairs.append((here, leaf * sub_count + (sub ^ 1)))
    return lax.ppermute(values, ("leaf", "sub"), pairs)


def bits_of(count):
    bits = []
    while count > 1:
        count = count // 2
        bits.append(count)
    return bits


def levels_of(subtree):
    sizes = []
    while subtree >= 1:
        sizes.append(subtree)
        subtree = subtree // 2
    starts = [sum(sizes[:number]) for number in range(len(sizes))]
    return sizes, starts


def halves(values):
    high = values.astype(jnp.bfloat16)
    return high, (values - high.astype(jnp.float32)).astype(jnp.bfloat16)


def dot(left, right, contract=((1,), (0,))):
    return lax.dot_general(left, right, (contract, ((), ())), preferred_element_type=jnp.float32)


def expand_kernel(
    leaf_count, targets_in, alive_in, vectors_in, basis_in, transfer_in, coupling_in, keep, send, own, *scratch
):
    targets, alive, vectors, basis, transfer, coupling, done, *sums = scratch
    subtree, rank, leaf_size = basis.shape
    clusters, far_count = coupling.shape[:2]
    nodes = leaf_count * clusters
    sizes, starts = levels_of(subtree)
    rows = vectors.shape[0]
    parity = lax.axis_index("leaf") % 2
    copies = [
        pltpu.make_async_copy(source, target, done.at[number])
        for number, (source, target) in enumerate(
            (
                (vectors_in, vectors),
                (basis_in, basis),
                (coupling_in.at[:subtree], coupling.at[:subtree]),
                (transfer_in, transfer),
                (targets_in, targets),
                (alive_in, alive),
                (coupling_in.at[subtree:], coupling.at[subtree:]),
            )
        )
    ]
    for copy in copies:
        copy.start()
    zero = jnp.zeros((rows, rank), jnp.float32)
    shared = len(sums) < clusters
    if shared:

        def clear(row, carry):
            sums[0][row] = zero
            return carry

        lax.fori_loop(0, nodes, clear, 0)
    else:
        for number, size in enumerate(sizes):
            for c in range(starts[number], starts[number] + size):
                for tree in range(leaf_count):
                    for j in range(starts[number], starts[number] + size):
                        sums[c][tree * clusters + j] = zero
    copies[0].wait()
    own[...] = vectors[...]
    copies[1].wait()
    hats = [
        dot(vectors[:, j * leaf_size : (j + 1) * leaf_size], basis[j], ((1,), (1,)))
        for j in range(subtree)
    ]
    copies[3].wait()
    for number in range(len(sizes) - 1):
        for p in range(sizes[number + 1]):
            total = None
            for c in (starts[number] + 2 * p, starts[number] + 2 * p + 1):
                high, low = halves(hats[c])
                part = dot(high, transfer[c]) + dot(low, transfer[c])
                total = part if total is None else total + part
            hats.append(total)
    lefts = [hat.astype(jnp.bfloat16) for hat in hats]
    copies[4].wait()
    copies[5].wait()
    for wait, members in ((2, range(subtree)), (6, range(subtree, clusters))):
        copies[wait].wait()
        for k in range(far_count):
            for c in members:
                term = dot(lefts[c], coupling[c, k])
                row = jnp.where(alive[c, k] == 1, targets[c, k], nodes)
                held = sums[0 if shared else c]
                held[row] = held[row] + term
    per = LANES // rank

    def gathered(tree):
        groups = []
        for first in range(0, clusters, per):
            lanes = []
            for place in range(first, first + per):
                if place >= clusters:
                    lanes.append(zero)
                    continue
                number = max(n for n in range(len(sizes)) if starts[n] <= place)
                row = tree * clusters + place
                if shared:
                    lanes.append(sums[0][row])
                else:
                    level = range(starts[number], starts[number] + sizes[number])
                    lanes.append(sum(sums[c][row] for c in level))
            groups.append(jnp.concatenate(lanes, axis=1))
        return groups

    def emit(half, carry):
        for out, tree in ((keep, 2 * half + parity), (send, 2 * half + 1 - parity)):
            for number, group in enumerate(gathered(tree)):
                out[half, number] = group.astype(out.dtype)
        return carry

    if leaf_count <= 8:
        for half in range(leaf_count // 2):
            emit(half, 0)
    else:
        lax.fori_loop(0, leaf_count // 2, emit, 0)


def expand(vectors, basis, transfer, coupling, targets, alive):
    leaf_count = lax.axis_size("leaf")
    clusters, _, rank = coupling.shape[:3]
    rows = vectors.shape[0]
    nodes = leaf_count * clusters
    groups = -(-clusters * rank // LANES)
    shape = (leaf_count // 2, groups, rows, LANES)
    copies = clusters if nodes <= 128 else 1
    return pl.pallas_call(
        functools.partial(expand_kernel, leaf_count),
        out_shape=[
            jax.ShapeDtypeStruct(shape, jnp.float32),
            jax.ShapeDtypeStruct(shape, jnp.bfloat16),
            jax.ShapeDtypeStruct(vectors.shape, vectors.dtype),
        ],
        in_specs=[HBM] * 6,
        out_specs=[VMEM] * 3,
        scratch_shapes=[
            pltpu.SMEM(targets.shape, targets.dtype),
            pltpu.SMEM(alive.shape, alive.dtype),
            pltpu.VMEM(vectors.shape, vectors.dtype),
            pltpu.VMEM(basis.shape, basis.dtype),
            pltpu.VMEM(transfer.shape, transfer.dtype),
            pltpu.VMEM(coupling.shape, coupling.dtype),
            pltpu.SemaphoreType.DMA((7,)),
        ]
        + [pltpu.VMEM((nodes + 1, rows, rank), jnp.float32)] * copies,
        compiler_params=PARAMS,
        name="expand",
    )(
        *(
            pltpu.with_memory_space_constraint(value, pltpu.HBM)
            for value in (targets, alive, vectors, basis, transfer, coupling)
        )
    )


def operator_kernel(transfer, basis, high_out, low_out):
    subtree, rank, leaf_size = basis.shape
    sizes, starts = levels_of(subtree)
    high_out[...] = jnp.zeros(high_out.shape, high_out.dtype)
    low_out[...] = jnp.zeros(low_out.shape, low_out.dtype)
    for j in range(subtree):
        columns = slice(j * leaf_size, (j + 1) * leaf_size)
        parts = (basis[j],)
        c = j
        for number in range(len(sizes)):
            at = slice(c * rank, (c + 1) * rank)
            high_out[at, columns] = parts[0]
            if len(parts) > 1:
                low_out[at, columns] = parts[1]
            if number + 1 < len(sizes):
                total = sum(dot(transfer[c], part, ((0,), (0,))) for part in parts)
                parts = halves(total)
                c = starts[number + 1] + (c - starts[number]) // 2


def operator(transfer, basis, depth):
    subtree, _, leaf_size = basis.shape
    shape = jax.ShapeDtypeStruct((depth, subtree * leaf_size), jnp.bfloat16)
    return pl.pallas_call(
        operator_kernel,
        out_shape=[shape, shape],
        in_specs=[VMEM, VMEM],
        out_specs=[VMEM, VMEM],
        compiler_params=PARAMS,
        name="operator",
    )(transfer, basis)


def near_kernel(places, sub_count, columns, alive, blocks, *refs):
    window, outs, pieces = refs[-1], refs[-1 - len(places) : -1], refs[: -1 - len(places)]
    per_tree = len(pieces) // 3
    rows, points = pieces[0].shape
    count, leaf_size = blocks.shape[1:3]
    subtree = points // leaf_size
    for tree in range(3):
        for part in range(per_tree):
            window[tree, part * rows : (part + 1) * rows, :] = pieces[tree * per_tree + part][...]
    me = lax.axis_index("leaf")
    first = me * subtree
    partner = (me ^ 1) * subtree
    total = None
    for k in range(count):
        column = columns[0, k]
        own_tree = (column >= first) & (column < first + subtree)
        partner_tree = (column >= partner) & (column < partner + subtree)
        tree = jnp.where(own_tree, 0, jnp.where(partner_tree, 1, 2))
        place = lax.rem(column, subtree)
        start = pl.multiple_of(place * leaf_size, leaf_size)
        taken = window[tree, :, pl.ds(start, leaf_size)]
        live = alive[0, k].astype(jnp.float32).astype(jnp.bfloat16)
        product = dot(taken * live, blocks[0, k])
        total = product if total is None else total + product
    size = total.shape[0] // sub_count
    for out, groups in zip(outs, places):
        for number, group in enumerate(groups):
            out[number] = total[group * size : (group + 1) * size].astype(out.dtype)


def near(pieces, blocks, columns, alive, rows, places):
    sub_count = lax.axis_size("sub")
    leaf_size = blocks.shape[2]
    points = pieces[0].shape[1]
    return pl.pallas_call(
        functools.partial(near_kernel, places, sub_count),
        out_shape=[
            jax.ShapeDtypeStruct(
                (len(groups), rows, leaf_size), jnp.bfloat16 if number else jnp.float32
            )
            for number, groups in enumerate(places)
        ],
        in_specs=[SMEM, SMEM] + [VMEM] * (1 + len(pieces)),
        out_specs=[VMEM] * len(places),
        scratch_shapes=[pltpu.VMEM((3, rows * sub_count, points), jnp.bfloat16)],
        compiler_params=PARAMS,
        name="near",
    )(columns, alive, blocks, *pieces)


def finish_kernel(sources, keep, got, high_in, low_in, *refs):
    nears, out = refs[:-1], refs[-1]
    incoming = jnp.concatenate(
        [keep[0, g] + got[0, g].astype(jnp.float32) for g in range(keep.shape[1])], axis=1
    )
    high, low = halves(incoming)
    far = dot(high, high_in[...]) + dot(low, high_in[...]) + dot(high, low_in[...])
    me = lax.axis_index("sub")
    leaf_size = nears[0].shape[2]
    pieces = [(source, nears[at][row].astype(jnp.float32)) for source, at, row in sources]
    for j in range(len(sources)):
        piece = pieces[0][1]
        for source, values in pieces[1:]:
            piece = jnp.where((me ^ source) == j, values, piece)
        columns = slice(j * leaf_size, (j + 1) * leaf_size)
        out[:, columns] = (piece + far[:, columns]).astype(out.dtype)


def finish(keep, got, high, low, nears, sources):
    rows = nears[0].shape[1]
    return pl.pallas_call(
        functools.partial(finish_kernel, sources),
        out_shape=jax.ShapeDtypeStruct((rows, high.shape[1]), jnp.bfloat16),
        in_specs=[VMEM] * (4 + len(nears)),
        out_specs=VMEM,
        compiler_params=PARAMS,
        name="finish",
    )(keep, got, high, low, *nears)


def local(
    vectors,
    near_blocks,
    near_cols,
    near_mask,
    leaf_basis,
    transfer,
    coupling,
    far_targets,
    far_mask,
):
    leaf_count = lax.axis_size("leaf")
    sub_count = lax.axis_size("sub")
    me = lax.axis_index("leaf")
    rows = vectors.shape[0]
    bits = bits_of(sub_count)
    keep, send, own = expand(vectors, leaf_basis, transfer, coupling, far_targets, far_mask)
    pair = jnp.concatenate([own, flip(vectors, "sub", bits[0])], axis=0)
    trees = [[pair], [flip(pair, "leaf", 1)], [beside(pair)]]
    got = flip(send, "leaf", 1)
    order = [0, bits[0]]
    for bit in bits[1:]:
        trees = [parts + [flip(part, "sub", bit) for part in parts] for parts in trees]
        order = order + [number ^ bit for number in order]
    pieces = [part for parts in trees for part in parts]
    high, low = operator(transfer, leaf_basis, keep.shape[1] * LANES)
    for size in bits_of(leaf_count)[:-1]:
        total = (keep + got.astype(keep.dtype)).reshape(2, size // 2, *keep.shape[1:])
        mine = (me & size) // size
        keep = lax.dynamic_index_in_dim(total, mine, 0, keepdims=False)
        send = lax.dynamic_index_in_dim(total, 1 - mine, 0, keepdims=False)
        got = flip(send.astype(jnp.bfloat16), "leaf", size)
    places = [[order.index(0)]] + [
        [order.index(home) for home in range(bit, 2 * bit)] for bit in bits
    ]
    made = near(pieces, near_blocks, near_cols, near_mask, rows, places)
    arrays = list(made)
    pool = {0: [(0, 0, 0)]}
    for number, bit in enumerate(bits):
        for row in range(bit):
            pool[bit + row] = [(0, number + 1, row)]
    for bit in bits:
        sent = [(home, item) for home in range(bit, 2 * bit) for item in pool[home]]
        if len(sent) == arrays[sent[0][1][1]].shape[0]:
            stack = arrays[sent[0][1][1]]
        else:
            stack = jnp.concatenate([arrays[at][row : row + 1] for _, (_, at, row) in sent], axis=0)
        arrays.append(flip(stack, "sub", bit))
        for row, (home, (source, _, _)) in enumerate(sent):
            pool[home ^ bit].append((source ^ bit, len(arrays) - 1, row))
    used = sorted({at for _, at, _ in pool[0]})
    sources = [(source, used.index(at), row) for source, at, row in pool[0]]
    return finish(keep, got, high, low, [arrays[at] for at in used], sources)


def solution(mesh):
    return jax.shard_map(
        local,
        mesh=mesh,
        in_specs=(
            P("sub", "leaf"),
            P(("leaf", "sub"), None, None, None),
            P(("leaf", "sub"), None),
            P(("leaf", "sub"), None),
            P("leaf", None, None),
            P("leaf", None, None),
            P("leaf", None, None, None),
            P("leaf", None),
            P("leaf", None),
        ),
        out_specs=P("sub", "leaf"),
        check_vma=False,
    )
```

```python
import functools

import jax
import jax.numpy as jnp
from jax import lax
from jax.experimental import pallas as pl
from jax.experimental.pallas import tpu as pltpu
from jax.sharding import PartitionSpec as P


LANES = 128
PARAMS = pltpu.CompilerParams(vmem_limit_bytes=16 * 2**20)
SMEM = pl.BlockSpec(memory_space=pltpu.SMEM)
VMEM = pl.BlockSpec(memory_space=pltpu.VMEM)
HBM = pl.BlockSpec(memory_space=pltpu.HBM)


def flip(values, axis, bit):
    count = lax.axis_size(axis)
    return lax.ppermute(values, axis, [(i, i ^ bit) for i in range(count)])


def beside(values):
    leaf_count, sub_count = lax.axis_size("leaf"), lax.axis_size("sub")
    pairs = []
    for leaf in range(leaf_count):
        other = ((leaf + 1) ^ 1) - 1
        for sub in range(sub_count):
            here = leaf * sub_count + sub
            if 0 <= other < leaf_count:
                pairs.append((here, other * sub_count + sub))
            else:
                pairs.append((here, leaf * sub_count + (sub ^ 1)))
    return lax.ppermute(values, ("leaf", "sub"), pairs)


def bits_of(count):
    bits = []
    while count > 1:
        count = count // 2
        bits.append(count)
    return bits


def levels_of(subtree):
    sizes = []
    while subtree >= 1:
        sizes.append(subtree)
        subtree = subtree // 2
    starts = [sum(sizes[:number]) for number in range(len(sizes))]
    return sizes, starts


def halves(values):
    high = values.astype(jnp.bfloat16)
    return high, (values - high.astype(jnp.float32)).astype(jnp.bfloat16)


def dot(left, right, contract=((1,), (0,))):
    return lax.dot_general(left, right, (contract, ((), ())), preferred_element_type=jnp.float32)


def expand_kernel(
    leaf_count, targets_in, alive_in, vectors_in, basis_in, transfer_in, coupling_in, keep, send, own, *scratch
):
    targets, alive, vectors, basis, transfer, coupling, done, *sums = scratch
    subtree, rank, leaf_size = basis.shape
    clusters, far_count = coupling.shape[:2]
    nodes = leaf_count * clusters
    sizes, starts = levels_of(subtree)
    rows = vectors.shape[0]
    parity = lax.axis_index("leaf") % 2
    copies = [
        pltpu.make_async_copy(source, target, done.at[number])
        for number, (source, target) in enumerate(
            (
                (vectors_in, vectors),
                (basis_in, basis),
                (coupling_in.at[:subtree], coupling.at[:subtree]),
                (transfer_in, transfer),
                (targets_in, targets),
                (alive_in, alive),
                (coupling_in.at[subtree:], coupling.at[subtree:]),
            )
        )
    ]
    for copy in copies:
        copy.start()
    zero = jnp.zeros((rows, rank), jnp.float32)
    shared = len(sums) < clusters
    if shared:

        def clear(row, carry):
            sums[0][row] = zero
            return carry

        lax.fori_loop(0, nodes, clear, 0)
    else:
        for number, size in enumerate(sizes):
            for c in range(starts[number], starts[number] + size):
                for tree in range(leaf_count):
                    for j in range(starts[number], starts[number] + size):
                        sums[c][tree * clusters + j] = zero
    copies[0].wait()
    own[...] = vectors[...]
    copies[1].wait()
    hats = [
        dot(vectors[:, j * leaf_size : (j + 1) * leaf_size], basis[j], ((1,), (1,)))
        for j in range(subtree)
    ]
    copies[3].wait()
    for number in range(len(sizes) - 1):
        for p in range(sizes[number + 1]):
            total = None
            for c in (starts[number] + 2 * p, starts[number] + 2 * p + 1):
                high, low = halves(hats[c])
                part = dot(high, transfer[c]) + dot(low, transfer[c])
                total = part if total is None else total + part
            hats.append(total)
    lefts = [hat.astype(jnp.bfloat16) for hat in hats]
    copies[4].wait()
    copies[5].wait()
    for wait, members in ((2, range(subtree)), (6, range(subtree, clusters))):
        copies[wait].wait()
        for k in range(far_count):
            for c in members:
                term = dot(lefts[c], coupling[c, k])
                row = jnp.where(alive[c, k] == 1, targets[c, k], nodes)
                held = sums[0 if shared else c]
                held[row] = held[row] + term
    per = LANES // rank

    def gathered(tree):
        groups = []
        for first in range(0, clusters, per):
            lanes = []
            for place in range(first, first + per):
                if place >= clusters:
                    lanes.append(zero)
                    continue
                number = max(n for n in range(len(sizes)) if starts[n] <= place)
                row = tree * clusters + place
                if shared:
                    lanes.append(sums[0][row])
                else:
                    level = range(starts[number], starts[number] + sizes[number])
                    lanes.append(sum(sums[c][row] for c in level))
            groups.append(jnp.concatenate(lanes, axis=1))
        return groups

    def emit(half, carry):
        for out, tree in ((keep, 2 * half + parity), (send, 2 * half + 1 - parity)):
            for number, group in enumerate(gathered(tree)):
                out[half, number] = group.astype(out.dtype)
        return carry

    if leaf_count <= 8:
        for half in range(leaf_count // 2):
            emit(half, 0)
    else:
        lax.fori_loop(0, leaf_count // 2, emit, 0)


def expand(vectors, basis, transfer, coupling, targets, alive):
    leaf_count = lax.axis_size("leaf")
    clusters, _, rank = coupling.shape[:3]
    rows = vectors.shape[0]
    nodes = leaf_count * clusters
    groups = -(-clusters * rank // LANES)
    shape = (leaf_count // 2, groups, rows, LANES)
    copies = clusters if nodes <= 128 else 1
    return pl.pallas_call(
        functools.partial(expand_kernel, leaf_count),
        out_shape=[
            jax.ShapeDtypeStruct(shape, jnp.float32),
            jax.ShapeDtypeStruct(shape, jnp.bfloat16),
            jax.ShapeDtypeStruct(vectors.shape, vectors.dtype),
        ],
        in_specs=[HBM] * 6,
        out_specs=[VMEM] * 3,
        scratch_shapes=[
            pltpu.SMEM(targets.shape, targets.dtype),
            pltpu.SMEM(alive.shape, alive.dtype),
            pltpu.VMEM(vectors.shape, vectors.dtype),
            pltpu.VMEM(basis.shape, basis.dtype),
            pltpu.VMEM(transfer.shape, transfer.dtype),
            pltpu.VMEM(coupling.shape, coupling.dtype),
            pltpu.SemaphoreType.DMA((7,)),
        ]
        + [pltpu.VMEM((nodes + 1, rows, rank), jnp.float32)] * copies,
        compiler_params=PARAMS,
        name="expand",
    )(
        *(
            pltpu.with_memory_space_constraint(value, pltpu.HBM)
            for value in (targets, alive, vectors, basis, transfer, coupling)
        )
    )


def operator_kernel(transfer, basis, high_out, low_out):
    subtree, rank, leaf_size = basis.shape
    sizes, starts = levels_of(subtree)
    high_out[...] = jnp.zeros(high_out.shape, high_out.dtype)
    low_out[...] = jnp.zeros(low_out.shape, low_out.dtype)
    for j in range(subtree):
        columns = slice(j * leaf_size, (j + 1) * leaf_size)
        parts = (basis[j],)
        c = j
        for number in range(len(sizes)):
            at = slice(c * rank, (c + 1) * rank)
            high_out[at, columns] = parts[0]
            if len(parts) > 1:
                low_out[at, columns] = parts[1]
            if number + 1 < len(sizes):
                total = sum(dot(transfer[c], part, ((0,), (0,))) for part in parts)
                parts = halves(total)
                c = starts[number + 1] + (c - starts[number]) // 2


def operator(transfer, basis, depth):
    subtree, _, leaf_size = basis.shape
    shape = jax.ShapeDtypeStruct((depth, subtree * leaf_size), jnp.bfloat16)
    return pl.pallas_call(
        operator_kernel,
        out_shape=[shape, shape],
        in_specs=[VMEM, VMEM],
        out_specs=[VMEM, VMEM],
        compiler_params=PARAMS,
        name="operator",
    )(transfer, basis)


def arrange_kernel(columns, alive, blocks, out):
    count, leaf_size = blocks.shape[1:3]
    subtree = (out.shape[0] - 1) // 3
    me = lax.axis_index("leaf")
    first = me * subtree
    partner = (me ^ 1) * subtree
    zero = jnp.zeros((leaf_size, blocks.shape[3]), out.dtype)
    for place in range(3 * subtree):
        out[place] = zero
    for k in range(count):
        column = columns[0, k]
        own_tree = (column >= first) & (column < first + subtree)
        partner_tree = (column >= partner) & (column < partner + subtree)
        tree = jnp.where(own_tree, 0, jnp.where(partner_tree, 1, 2))
        place = tree * subtree + lax.rem(column, subtree)
        out[jnp.where(alive[0, k] == 1, place, 3 * subtree)] = blocks[0, k]


def arrange(blocks, columns, alive, subtree):
    return pl.pallas_call(
        arrange_kernel,
        out_shape=jax.ShapeDtypeStruct((3 * subtree + 1, *blocks.shape[2:]), blocks.dtype),
        in_specs=[SMEM, SMEM, VMEM],
        out_specs=VMEM,
        compiler_params=PARAMS,
        name="arrange",
    )(columns, alive, blocks)


def near_kernel(places, sub_count, blocks, *refs):
    outs, pieces = refs[-len(places) :], refs[: -len(places)]
    middles, outers = pieces[0::2], pieces[1::2]
    rows, points = middles[0].shape
    leaf_size = blocks.shape[1]
    subtree = points // leaf_size
    total = None
    for tree in range(3):
        for j in range(subtree):
            columns = slice(j * leaf_size, (j + 1) * leaf_size)
            if tree == 0:
                taken = [ref[:, columns] for ref in middles]
            else:
                taken = [ref[(tree - 1) * rows : tree * rows, columns] for ref in outers]
            product = dot(jnp.concatenate(taken, axis=0), blocks[tree * subtree + j])
            total = product if total is None else total + product
    size = total.shape[0] // sub_count
    for out, groups in zip(outs, places):
        for number, group in enumerate(groups):
            out[number] = total[group * size : (group + 1) * size].astype(out.dtype)


def near(pieces, blocks, rows, places):
    sub_count = lax.axis_size("sub")
    leaf_size = blocks.shape[1]
    flat = [array for pair in pieces for array in pair]
    return pl.pallas_call(
        functools.partial(near_kernel, places, sub_count),
        out_shape=[
            jax.ShapeDtypeStruct(
                (len(groups), rows, leaf_size), jnp.bfloat16 if number else jnp.float32
            )
            for number, groups in enumerate(places)
        ],
        in_specs=[VMEM] * (1 + len(flat)),
        out_specs=[VMEM] * len(places),
        compiler_params=PARAMS,
        name="near",
    )(blocks, *flat)


def far_kernel(keep, got, high_in, low_in, out):
    incoming = jnp.concatenate(
        [keep[0, g] + got[0, g].astype(jnp.float32) for g in range(keep.shape[1])], axis=1
    )
    high, low = halves(incoming)
    rows = high.shape[0]
    both = dot(jnp.concatenate([high, low], axis=0), high_in[...])
    out[...] = both[:rows] + both[rows:] + dot(high, low_in[...])


def far(keep, got, high, low):
    return pl.pallas_call(
        far_kernel,
        out_shape=jax.ShapeDtypeStruct((keep.shape[2], high.shape[1]), jnp.float32),
        in_specs=[VMEM] * 4,
        out_specs=VMEM,
        compiler_params=PARAMS,
        name="far",
    )(keep, got, high, low)


def finish_kernel(sources, far_in, *refs):
    nears, out = refs[:-1], refs[-1]
    me = lax.axis_index("sub")
    leaf_size = nears[0].shape[2]
    pieces = [(source, nears[at][row].astype(jnp.float32)) for source, at, row in sources]
    for j in range(len(sources)):
        piece = pieces[0][1]
        for source, values in pieces[1:]:
            piece = jnp.where((me ^ source) == j, values, piece)
        columns = slice(j * leaf_size, (j + 1) * leaf_size)
        out[:, columns] = (piece + far_in[:, columns]).astype(out.dtype)


def finish(far_part, nears, sources):
    return pl.pallas_call(
        functools.partial(finish_kernel, sources),
        out_shape=jax.ShapeDtypeStruct(far_part.shape, jnp.bfloat16),
        in_specs=[VMEM] * (1 + len(nears)),
        out_specs=VMEM,
        compiler_params=PARAMS,
        name="finish",
    )(far_part, *nears)


def local(
    vectors,
    near_blocks,
    near_cols,
    near_mask,
    leaf_basis,
    transfer,
    coupling,
    far_targets,
    far_mask,
):
    leaf_count = lax.axis_size("leaf")
    sub_count = lax.axis_size("sub")
    me = lax.axis_index("leaf")
    rows = vectors.shape[0]
    bits = bits_of(sub_count)
    keep, send, own = expand(vectors, leaf_basis, transfer, coupling, far_targets, far_mask)
    pair = jnp.concatenate([own, flip(vectors, "sub", bits[0])], axis=0)
    sides = jnp.concatenate([flip(pair, "leaf", 1), beside(pair)], axis=0)
    got = flip(send, "leaf", 1)
    order = [0, bits[0]]
    pieces = [(pair, sides)]
    for bit in bits[1:]:
        pieces = pieces + [
            (flip(middle, "sub", bit), flip(outer, "sub", bit))
            for middle, outer in pieces
        ]
        order = order + [number ^ bit for number in order]
    high, low = operator(transfer, leaf_basis, keep.shape[1] * LANES)
    for size in bits_of(leaf_count)[:-1]:
        total = (keep + got.astype(keep.dtype)).reshape(2, size // 2, *keep.shape[1:])
        mine = (me & size) // size
        keep = lax.dynamic_index_in_dim(total, mine, 0, keepdims=False)
        send = lax.dynamic_index_in_dim(total, 1 - mine, 0, keepdims=False)
        got = flip(send.astype(jnp.bfloat16), "leaf", size)
    places = [[order.index(0)]] + [
        [order.index(home) for home in range(bit, 2 * bit)] for bit in bits
    ]
    blocks = arrange(near_blocks, near_cols, near_mask, leaf_basis.shape[0])
    made = near(pieces, blocks, rows, places)
    arrays = list(made)
    pool = {0: [(0, 0, 0)]}
    for number, bit in enumerate(bits):
        for row in range(bit):
            pool[bit + row] = [(0, number + 1, row)]
    for bit in bits:
        sent = [(home, item) for home in range(bit, 2 * bit) for item in pool[home]]
        if len(sent) == arrays[sent[0][1][1]].shape[0]:
            stack = arrays[sent[0][1][1]]
        else:
            stack = jnp.concatenate([arrays[at][row : row + 1] for _, (_, at, row) in sent], axis=0)
        arrays.append(flip(stack, "sub", bit))
        for row, (home, (source, _, _)) in enumerate(sent):
            pool[home ^ bit].append((source ^ bit, len(arrays) - 1, row))
    used = sorted({at for _, at, _ in pool[0]})
    sources = [(source, used.index(at), row) for source, at, row in pool[0]]
    far_part = far(keep, got, high, low)
    return finish(far_part, [arrays[at] for at in used], sources)


def solution(mesh):
    return jax.shard_map(
        local,
        mesh=mesh,
        in_specs=(
            P("sub", "leaf"),
            P(("leaf", "sub"), None, None, None),
            P(("leaf", "sub"), None),
            P(("leaf", "sub"), None),
            P("leaf", None, None),
            P("leaf", None, None),
            P("leaf", None, None, None),
            P("leaf", None),
            P("leaf", None),
        ),
        out_specs=P("sub", "leaf"),
        check_vma=False,
    )
```

```python
import functools

import jax
import jax.numpy as jnp
from jax import lax
from jax.experimental import pallas as pl
from jax.experimental.pallas import tpu as pltpu
from jax.sharding import PartitionSpec as P


LANES = 128
PARAMS = pltpu.CompilerParams(vmem_limit_bytes=16 * 2**20)
SMEM = pl.BlockSpec(memory_space=pltpu.SMEM)
VMEM = pl.BlockSpec(memory_space=pltpu.VMEM)
HBM = pl.BlockSpec(memory_space=pltpu.HBM)


def flip(values, axis, bit):
    count = lax.axis_size(axis)
    return lax.ppermute(values, axis, [(i, i ^ bit) for i in range(count)])


def beside(values):
    leaf_count, sub_count = lax.axis_size("leaf"), lax.axis_size("sub")
    pairs = []
    for leaf in range(leaf_count):
        other = ((leaf + 1) ^ 1) - 1
        for sub in range(sub_count):
            here = leaf * sub_count + sub
            if 0 <= other < leaf_count:
                pairs.append((here, other * sub_count + sub))
            else:
                pairs.append((here, leaf * sub_count + (sub ^ 1)))
    return lax.ppermute(values, ("leaf", "sub"), pairs)


def bits_of(count):
    bits = []
    while count > 1:
        count = count // 2
        bits.append(count)
    return bits


def stages_of(leaf_count):
    bits = bits_of(leaf_count)[::-1]
    return bits[1:] + bits[:1]


def levels_of(subtree):
    sizes = []
    while subtree >= 1:
        sizes.append(subtree)
        subtree = subtree // 2
    starts = [sum(sizes[:number]) for number in range(len(sizes))]
    return sizes, starts


def halves(values):
    high = values.astype(jnp.bfloat16)
    return high, (values - high.astype(jnp.float32)).astype(jnp.bfloat16)


def dot(left, right, contract=((1,), (0,))):
    return lax.dot_general(left, right, (contract, ((), ())), preferred_element_type=jnp.float32)


def expand_kernel(
    leaf_count, targets_in, alive_in, vectors_in, basis_in, transfer_in, coupling_in, keep, send, own, *scratch
):
    targets, alive, vectors, basis, transfer, coupling, done, *sums = scratch
    subtree, rank, leaf_size = basis.shape
    clusters, far_count = coupling.shape[:2]
    nodes = leaf_count * clusters
    sizes, starts = levels_of(subtree)
    rows = vectors.shape[0]
    bit = stages_of(leaf_count)[0]
    mine = (lax.axis_index("leaf") & bit) // bit
    copies = [
        pltpu.make_async_copy(source, target, done.at[number])
        for number, (source, target) in enumerate(
            (
                (vectors_in, vectors),
                (basis_in, basis),
                (coupling_in.at[:subtree], coupling.at[:subtree]),
                (transfer_in, transfer),
                (targets_in, targets),
                (alive_in, alive),
                (coupling_in.at[subtree:], coupling.at[subtree:]),
            )
        )
    ]
    for copy in copies:
        copy.start()
    zero = jnp.zeros((rows, rank), jnp.float32)
    shared = len(sums) < clusters
    if shared:

        def clear(row, carry):
            sums[0][row] = zero
            return carry

        lax.fori_loop(0, nodes, clear, 0)
    else:
        for number, size in enumerate(sizes):
            for c in range(starts[number], starts[number] + size):
                for tree in range(leaf_count):
                    for j in range(starts[number], starts[number] + size):
                        sums[c][tree * clusters + j] = zero
    copies[0].wait()
    own[...] = vectors[...]
    copies[1].wait()
    hats = [
        dot(vectors[:, j * leaf_size : (j + 1) * leaf_size], basis[j], ((1,), (1,)))
        for j in range(subtree)
    ]
    copies[3].wait()
    for number in range(len(sizes) - 1):
        for p in range(sizes[number + 1]):
            total = None
            for c in (starts[number] + 2 * p, starts[number] + 2 * p + 1):
                high, low = halves(hats[c])
                part = dot(high, transfer[c]) + dot(low, transfer[c])
                total = part if total is None else total + part
            hats.append(total)
    lefts = [hat.astype(jnp.bfloat16) for hat in hats]
    copies[4].wait()
    copies[5].wait()
    for wait, members in ((2, range(subtree)), (6, range(subtree, clusters))):
        copies[wait].wait()
        for k in range(far_count):
            for c in members:
                term = dot(lefts[c], coupling[c, k])
                row = jnp.where(alive[c, k] == 1, targets[c, k], nodes)
                held = sums[0 if shared else c]
                held[row] = held[row] + term
    per = LANES // rank

    def gathered(tree):
        groups = []
        for first in range(0, clusters, per):
            lanes = []
            for place in range(first, first + per):
                if place >= clusters:
                    lanes.append(zero)
                    continue
                number = max(n for n in range(len(sizes)) if starts[n] <= place)
                row = tree * clusters + place
                if shared:
                    lanes.append(sums[0][row])
                else:
                    level = range(starts[number], starts[number] + sizes[number])
                    lanes.append(sum(sums[c][row] for c in level))
            groups.append(jnp.concatenate(lanes, axis=1))
        return groups

    def emit(half, carry):
        first = (half // bit) * 2 * bit + half % bit
        for out, tree in ((keep, first + mine * bit), (send, first + (1 - mine) * bit)):
            for number, group in enumerate(gathered(tree)):
                out[half, number] = group.astype(out.dtype)
        return carry

    if leaf_count <= 8:
        for half in range(leaf_count // 2):
            emit(half, 0)
    else:
        lax.fori_loop(0, leaf_count // 2, emit, 0)


def expand(vectors, basis, transfer, coupling, targets, alive):
    leaf_count = lax.axis_size("leaf")
    clusters, _, rank = coupling.shape[:3]
    rows = vectors.shape[0]
    nodes = leaf_count * clusters
    groups = -(-clusters * rank // LANES)
    shape = (leaf_count // 2, groups, rows, LANES)
    copies = clusters if nodes <= 128 else 1
    return pl.pallas_call(
        functools.partial(expand_kernel, leaf_count),
        out_shape=[
            jax.ShapeDtypeStruct(shape, jnp.float32),
            jax.ShapeDtypeStruct(shape, jnp.bfloat16),
            jax.ShapeDtypeStruct(vectors.shape, vectors.dtype),
        ],
        in_specs=[HBM] * 6,
        out_specs=[VMEM] * 3,
        scratch_shapes=[
            pltpu.SMEM(targets.shape, targets.dtype),
            pltpu.SMEM(alive.shape, alive.dtype),
            pltpu.VMEM(vectors.shape, vectors.dtype),
            pltpu.VMEM(basis.shape, basis.dtype),
            pltpu.VMEM(transfer.shape, transfer.dtype),
            pltpu.VMEM(coupling.shape, coupling.dtype),
            pltpu.SemaphoreType.DMA((7,)),
        ]
        + [pltpu.VMEM((nodes + 1, rows, rank), jnp.float32)] * copies,
        compiler_params=PARAMS,
        name="expand",
    )(
        *(
            pltpu.with_memory_space_constraint(value, pltpu.HBM)
            for value in (targets, alive, vectors, basis, transfer, coupling)
        )
    )


def operator_kernel(transfer, basis, high_out, low_out):
    subtree, rank, leaf_size = basis.shape
    sizes, starts = levels_of(subtree)
    high_out[...] = jnp.zeros(high_out.shape, high_out.dtype)
    low_out[...] = jnp.zeros(low_out.shape, low_out.dtype)
    for j in range(subtree):
        columns = slice(j * leaf_size, (j + 1) * leaf_size)
        parts = (basis[j],)
        c = j
        for number in range(len(sizes)):
            at = slice(c * rank, (c + 1) * rank)
            high_out[at, columns] = parts[0]
            if len(parts) > 1:
                low_out[at, columns] = parts[1]
            if number + 1 < len(sizes):
                total = sum(dot(transfer[c], part, ((0,), (0,))) for part in parts)
                parts = halves(total)
                c = starts[number + 1] + (c - starts[number]) // 2


def operator(transfer, basis, depth):
    subtree, _, leaf_size = basis.shape
    shape = jax.ShapeDtypeStruct((depth, subtree * leaf_size), jnp.bfloat16)
    return pl.pallas_call(
        operator_kernel,
        out_shape=[shape, shape],
        in_specs=[VMEM, VMEM],
        out_specs=[VMEM, VMEM],
        compiler_params=PARAMS,
        name="operator",
    )(transfer, basis)


def arrange_kernel(columns, alive, blocks, out):
    count, leaf_size = blocks.shape[1:3]
    subtree = (out.shape[0] - 1) // 3
    me = lax.axis_index("leaf")
    first = me * subtree
    partner = (me ^ 1) * subtree
    zero = jnp.zeros((leaf_size, blocks.shape[3]), out.dtype)
    for place in range(3 * subtree):
        out[place] = zero
    for k in range(count):
        column = columns[0, k]
        own_tree = (column >= first) & (column < first + subtree)
        partner_tree = (column >= partner) & (column < partner + subtree)
        tree = jnp.where(own_tree, 0, jnp.where(partner_tree, 1, 2))
        place = tree * subtree + lax.rem(column, subtree)
        out[jnp.where(alive[0, k] == 1, place, 3 * subtree)] = blocks[0, k]


def arrange(blocks, columns, alive, subtree):
    return pl.pallas_call(
        arrange_kernel,
        out_shape=jax.ShapeDtypeStruct((3 * subtree + 1, *blocks.shape[2:]), blocks.dtype),
        in_specs=[SMEM, SMEM, VMEM],
        out_specs=VMEM,
        compiler_params=PARAMS,
        name="arrange",
    )(columns, alive, blocks)


def near_kernel(places, sub_count, blocks, *refs):
    outs, pieces = refs[-len(places) :], refs[: -len(places)]
    middles, outers = pieces[0::2], pieces[1::2]
    rows, points = middles[0].shape
    leaf_size = blocks.shape[1]
    subtree = points // leaf_size
    total = None
    for tree in range(3):
        for j in range(subtree):
            columns = slice(j * leaf_size, (j + 1) * leaf_size)
            if tree == 0:
                taken = [ref[:, columns] for ref in middles]
            else:
                taken = [ref[(tree - 1) * rows : tree * rows, columns] for ref in outers]
            product = dot(jnp.concatenate(taken, axis=0), blocks[tree * subtree + j])
            total = product if total is None else total + product
    size = total.shape[0] // sub_count
    for out, groups in zip(outs, places):
        for number, group in enumerate(groups):
            out[number] = total[group * size : (group + 1) * size].astype(out.dtype)


def near(pieces, blocks, rows, places):
    sub_count = lax.axis_size("sub")
    leaf_size = blocks.shape[1]
    flat = [array for pair in pieces for array in pair]
    return pl.pallas_call(
        functools.partial(near_kernel, places, sub_count),
        out_shape=[
            jax.ShapeDtypeStruct(
                (len(groups), rows, leaf_size), jnp.bfloat16 if number else jnp.float32
            )
            for number, groups in enumerate(places)
        ],
        in_specs=[VMEM] * (1 + len(flat)),
        out_specs=[VMEM] * len(places),
        compiler_params=PARAMS,
        name="near",
    )(blocks, *flat)


def far_kernel(keep, got, high_in, low_in, out):
    incoming = jnp.concatenate(
        [keep[0, g] + got[0, g].astype(jnp.float32) for g in range(keep.shape[1])], axis=1
    )
    high, low = halves(incoming)
    rows = high.shape[0]
    both = dot(jnp.concatenate([high, low], axis=0), high_in[...])
    out[...] = both[:rows] + both[rows:] + dot(high, low_in[...])


def far(keep, got, high, low):
    return pl.pallas_call(
        far_kernel,
        out_shape=jax.ShapeDtypeStruct((keep.shape[2], high.shape[1]), jnp.float32),
        in_specs=[VMEM] * 4,
        out_specs=VMEM,
        compiler_params=PARAMS,
        name="far",
    )(keep, got, high, low)


def finish_kernel(sources, far_in, *refs):
    nears, out = refs[:-1], refs[-1]
    me = lax.axis_index("sub")
    leaf_size = nears[0].shape[2]
    pieces = [(source, nears[at][row].astype(jnp.float32)) for source, at, row in sources]
    for j in range(len(sources)):
        piece = pieces[0][1]
        for source, values in pieces[1:]:
            piece = jnp.where((me ^ source) == j, values, piece)
        columns = slice(j * leaf_size, (j + 1) * leaf_size)
        out[:, columns] = (piece + far_in[:, columns]).astype(out.dtype)


def finish(far_part, nears, sources):
    return pl.pallas_call(
        functools.partial(finish_kernel, sources),
        out_shape=jax.ShapeDtypeStruct(far_part.shape, jnp.bfloat16),
        in_specs=[VMEM] * (1 + len(nears)),
        out_specs=VMEM,
        compiler_params=PARAMS,
        name="finish",
    )(far_part, *nears)


def local(
    vectors,
    near_blocks,
    near_cols,
    near_mask,
    leaf_basis,
    transfer,
    coupling,
    far_targets,
    far_mask,
):
    leaf_count = lax.axis_size("leaf")
    sub_count = lax.axis_size("sub")
    me = lax.axis_index("leaf")
    rows = vectors.shape[0]
    bits = bits_of(sub_count)
    keep, send, own = expand(vectors, leaf_basis, transfer, coupling, far_targets, far_mask)
    pair = jnp.concatenate([own, flip(vectors, "sub", bits[0])], axis=0)
    sides = jnp.concatenate([flip(pair, "leaf", 1), beside(pair)], axis=0)
    stages = stages_of(leaf_count)
    got = flip(send, "leaf", stages[0])
    order = [0, bits[0]]
    pieces = [(pair, sides)]
    for bit in bits[1:]:
        pieces = pieces + [
            (flip(middle, "sub", bit), flip(outer, "sub", bit))
            for middle, outer in pieces
        ]
        order = order + [number ^ bit for number in order]
    high, low = operator(transfer, leaf_basis, keep.shape[1] * LANES)
    for bit in sorted(stages[1:], reverse=True):
        total = (keep + got.astype(keep.dtype)).reshape(2, -1, *keep.shape[1:])
        mine = (me & bit) // bit
        keep = lax.dynamic_index_in_dim(total, mine, 0, keepdims=False)
        send = lax.dynamic_index_in_dim(total, 1 - mine, 0, keepdims=False)
        got = flip(send.astype(jnp.bfloat16), "leaf", bit)
    places = [[order.index(0)]] + [
        [order.index(home) for home in range(bit, 2 * bit)] for bit in bits
    ]
    blocks = arrange(near_blocks, near_cols, near_mask, leaf_basis.shape[0])
    made = near(pieces, blocks, rows, places)
    arrays = list(made)
    pool = {0: [(0, 0, 0)]}
    for number, bit in enumerate(bits):
        for row in range(bit):
            pool[bit + row] = [(0, number + 1, row)]
    for bit in bits:
        sent = [(home, item) for home in range(bit, 2 * bit) for item in pool[home]]
        if len(sent) == arrays[sent[0][1][1]].shape[0]:
            stack = arrays[sent[0][1][1]]
        else:
            stack = jnp.concatenate([arrays[at][row : row + 1] for _, (_, at, row) in sent], axis=0)
        arrays.append(flip(stack, "sub", bit))
        for row, (home, (source, _, _)) in enumerate(sent):
            pool[home ^ bit].append((source ^ bit, len(arrays) - 1, row))
    used = sorted({at for _, at, _ in pool[0]})
    sources = [(source, used.index(at), row) for source, at, row in pool[0]]
    far_part = far(keep, got, high, low)
    return finish(far_part, [arrays[at] for at in used], sources)


def solution(mesh):
    return jax.shard_map(
        local,
        mesh=mesh,
        in_specs=(
            P("sub", "leaf"),
            P(("leaf", "sub"), None, None, None),
            P(("leaf", "sub"), None),
            P(("leaf", "sub"), None),
            P("leaf", None, None),
            P("leaf", None, None),
            P("leaf", None, None, None),
            P("leaf", None),
            P("leaf", None),
        ),
        out_specs=P("sub", "leaf"),
        check_vma=False,
    )
```

```python
import functools

import jax
import jax.numpy as jnp
from jax import lax
from jax.experimental import pallas as pl
from jax.experimental.pallas import tpu as pltpu
from jax.sharding import PartitionSpec as P


LANES = 128
PARAMS = pltpu.CompilerParams(vmem_limit_bytes=16 * 2**20)
SMEM = pl.BlockSpec(memory_space=pltpu.SMEM)
VMEM = pl.BlockSpec(memory_space=pltpu.VMEM)
HBM = pl.BlockSpec(memory_space=pltpu.HBM)


def flip(values, axis, bit):
    count = lax.axis_size(axis)
    return lax.ppermute(values, axis, [(i, i ^ bit) for i in range(count)])


def across(values, partner, turn):
    leaf_count, sub_count = lax.axis_size("leaf"), lax.axis_size("sub")
    pairs = []
    for leaf in range(leaf_count):
        other = partner(leaf)
        inside = 0 <= other < leaf_count
        for sub in range(sub_count):
            here = leaf * sub_count + sub
            if inside:
                pairs.append((here, other * sub_count + (sub ^ turn)))
            else:
                pairs.append((here, leaf * sub_count + (sub ^ 1)))
    return lax.ppermute(values, ("leaf", "sub"), pairs)


def span_of(steps):
    numbers = [0]
    for step in steps:
        numbers = numbers + [number ^ step for number in numbers]
    return numbers


def bits_of(count):
    bits = []
    while count > 1:
        count = count // 2
        bits.append(count)
    return bits


def stages_of(leaf_count):
    bits = bits_of(leaf_count)[::-1]
    return bits[1:] + bits[:1]


def levels_of(subtree):
    sizes = []
    while subtree >= 1:
        sizes.append(subtree)
        subtree = subtree // 2
    starts = [sum(sizes[:number]) for number in range(len(sizes))]
    return sizes, starts


def halves(values):
    high = values.astype(jnp.bfloat16)
    return high, (values - high.astype(jnp.float32)).astype(jnp.bfloat16)


def dot(left, right, contract=((1,), (0,))):
    return lax.dot_general(left, right, (contract, ((), ())), preferred_element_type=jnp.float32)


def expand_kernel(
    leaf_count, targets_in, alive_in, vectors_in, basis_in, transfer_in, coupling_in, keep, send, own, *scratch
):
    targets, alive, vectors, basis, transfer, coupling, done, *sums = scratch
    subtree, rank, leaf_size = basis.shape
    clusters, far_count = coupling.shape[:2]
    nodes = leaf_count * clusters
    sizes, starts = levels_of(subtree)
    rows = vectors.shape[0]
    bit = stages_of(leaf_count)[0]
    mine = (lax.axis_index("leaf") & bit) // bit
    copies = [
        pltpu.make_async_copy(source, target, done.at[number])
        for number, (source, target) in enumerate(
            (
                (vectors_in, vectors),
                (basis_in, basis),
                (coupling_in.at[:subtree], coupling.at[:subtree]),
                (transfer_in, transfer),
                (targets_in, targets),
                (alive_in, alive),
                (coupling_in.at[subtree:], coupling.at[subtree:]),
            )
        )
    ]
    for copy in copies:
        copy.start()
    zero = jnp.zeros((rows, rank), jnp.float32)
    shared = len(sums) < clusters
    if shared:

        def clear(row, carry):
            sums[0][row] = zero
            return carry

        lax.fori_loop(0, nodes, clear, 0)
    else:
        for number, size in enumerate(sizes):
            for c in range(starts[number], starts[number] + size):
                for tree in range(leaf_count):
                    for j in range(starts[number], starts[number] + size):
                        sums[c][tree * clusters + j] = zero
    copies[0].wait()
    own[...] = vectors[...]
    copies[1].wait()
    hats = [
        dot(vectors[:, j * leaf_size : (j + 1) * leaf_size], basis[j], ((1,), (1,)))
        for j in range(subtree)
    ]
    copies[3].wait()
    for number in range(len(sizes) - 1):
        for p in range(sizes[number + 1]):
            total = None
            for c in (starts[number] + 2 * p, starts[number] + 2 * p + 1):
                high, low = halves(hats[c])
                part = dot(high, transfer[c]) + dot(low, transfer[c])
                total = part if total is None else total + part
            hats.append(total)
    lefts = [hat.astype(jnp.bfloat16) for hat in hats]
    copies[4].wait()
    copies[5].wait()
    for wait, members in ((2, range(subtree)), (6, range(subtree, clusters))):
        copies[wait].wait()
        for k in range(far_count):
            for c in members:
                term = dot(lefts[c], coupling[c, k])
                row = jnp.where(alive[c, k] == 1, targets[c, k], nodes)
                held = sums[0 if shared else c]
                held[row] = held[row] + term
    per = LANES // rank

    def gathered(tree):
        groups = []
        for first in range(0, clusters, per):
            lanes = []
            for place in range(first, first + per):
                if place >= clusters:
                    lanes.append(zero)
                    continue
                number = max(n for n in range(len(sizes)) if starts[n] <= place)
                row = tree * clusters + place
                if shared:
                    lanes.append(sums[0][row])
                else:
                    level = range(starts[number], starts[number] + sizes[number])
                    lanes.append(sum(sums[c][row] for c in level))
            groups.append(jnp.concatenate(lanes, axis=1))
        return groups

    def emit(half, carry):
        first = (half // bit) * 2 * bit + half % bit
        for out, tree in ((keep, first + mine * bit), (send, first + (1 - mine) * bit)):
            for number, group in enumerate(gathered(tree)):
                out[half, number] = group.astype(out.dtype)
        return carry

    if leaf_count <= 8:
        for half in range(leaf_count // 2):
            emit(half, 0)
    else:
        lax.fori_loop(0, leaf_count // 2, emit, 0)


def expand(vectors, basis, transfer, coupling, targets, alive):
    leaf_count = lax.axis_size("leaf")
    clusters, _, rank = coupling.shape[:3]
    rows = vectors.shape[0]
    nodes = leaf_count * clusters
    groups = -(-clusters * rank // LANES)
    shape = (leaf_count // 2, groups, rows, LANES)
    copies = clusters if nodes <= 128 else 1
    return pl.pallas_call(
        functools.partial(expand_kernel, leaf_count),
        out_shape=[
            jax.ShapeDtypeStruct(shape, jnp.float32),
            jax.ShapeDtypeStruct(shape, jnp.bfloat16),
            jax.ShapeDtypeStruct(vectors.shape, vectors.dtype),
        ],
        in_specs=[HBM] * 6,
        out_specs=[VMEM] * 3,
        scratch_shapes=[
            pltpu.SMEM(targets.shape, targets.dtype),
            pltpu.SMEM(alive.shape, alive.dtype),
            pltpu.VMEM(vectors.shape, vectors.dtype),
            pltpu.VMEM(basis.shape, basis.dtype),
            pltpu.VMEM(transfer.shape, transfer.dtype),
            pltpu.VMEM(coupling.shape, coupling.dtype),
            pltpu.SemaphoreType.DMA((7,)),
        ]
        + [pltpu.VMEM((nodes + 1, rows, rank), jnp.float32)] * copies,
        compiler_params=PARAMS,
        name="expand",
    )(
        *(
            pltpu.with_memory_space_constraint(value, pltpu.HBM)
            for value in (targets, alive, vectors, basis, transfer, coupling)
        )
    )


def operator_kernel(transfer, basis, high_out, low_out):
    subtree, rank, leaf_size = basis.shape
    sizes, starts = levels_of(subtree)
    high_out[...] = jnp.zeros(high_out.shape, high_out.dtype)
    low_out[...] = jnp.zeros(low_out.shape, low_out.dtype)
    for j in range(subtree):
        columns = slice(j * leaf_size, (j + 1) * leaf_size)
        parts = (basis[j],)
        c = j
        for number in range(len(sizes)):
            at = slice(c * rank, (c + 1) * rank)
            high_out[at, columns] = parts[0]
            if len(parts) > 1:
                low_out[at, columns] = parts[1]
            if number + 1 < len(sizes):
                total = sum(dot(transfer[c], part, ((0,), (0,))) for part in parts)
                parts = halves(total)
                c = starts[number + 1] + (c - starts[number]) // 2


def operator(transfer, basis, depth):
    subtree, _, leaf_size = basis.shape
    shape = jax.ShapeDtypeStruct((depth, subtree * leaf_size), jnp.bfloat16)
    return pl.pallas_call(
        operator_kernel,
        out_shape=[shape, shape],
        in_specs=[VMEM, VMEM],
        out_specs=[VMEM, VMEM],
        compiler_params=PARAMS,
        name="operator",
    )(transfer, basis)


def arrange_kernel(columns, alive, blocks, out):
    count, leaf_size = blocks.shape[1:3]
    subtree = (out.shape[0] - 1) // 3
    me = lax.axis_index("leaf")
    first = me * subtree
    partner = (me ^ 1) * subtree
    zero = jnp.zeros((leaf_size, blocks.shape[3]), out.dtype)
    for place in range(3 * subtree):
        out[place] = zero
    for k in range(count):
        column = columns[0, k]
        own_tree = (column >= first) & (column < first + subtree)
        partner_tree = (column >= partner) & (column < partner + subtree)
        tree = jnp.where(own_tree, 0, jnp.where(partner_tree, 1, 2))
        place = tree * subtree + lax.rem(column, subtree)
        out[jnp.where(alive[0, k] == 1, place, 3 * subtree)] = blocks[0, k]


def arrange(blocks, columns, alive, subtree):
    return pl.pallas_call(
        arrange_kernel,
        out_shape=jax.ShapeDtypeStruct((3 * subtree + 1, *blocks.shape[2:]), blocks.dtype),
        in_specs=[SMEM, SMEM, VMEM],
        out_specs=VMEM,
        compiler_params=PARAMS,
        name="arrange",
    )(columns, alive, blocks)


def near_kernel(places, sub_count, blocks, *refs):
    outs, pieces = refs[-len(places) :], refs[: -len(places)]
    middles, outers = pieces[0::2], pieces[1::2]
    rows, points = middles[0].shape
    leaf_size = blocks.shape[1]
    subtree = points // leaf_size
    total = None
    for tree in range(3):
        for j in range(subtree):
            columns = slice(j * leaf_size, (j + 1) * leaf_size)
            if tree == 0:
                taken = [ref[:, columns] for ref in middles]
            else:
                taken = [ref[(tree - 1) * rows : tree * rows, columns] for ref in outers]
            product = dot(jnp.concatenate(taken, axis=0), blocks[tree * subtree + j])
            total = product if total is None else total + product
    size = total.shape[0] // sub_count
    for out, groups in zip(outs, places):
        for number, group in enumerate(groups):
            out[number] = total[group * size : (group + 1) * size].astype(out.dtype)


def near(pieces, blocks, rows, places):
    sub_count = lax.axis_size("sub")
    leaf_size = blocks.shape[1]
    flat = [array for pair in pieces for array in pair]
    return pl.pallas_call(
        functools.partial(near_kernel, places, sub_count),
        out_shape=[
            jax.ShapeDtypeStruct(
                (len(groups), rows, leaf_size), jnp.bfloat16 if number else jnp.float32
            )
            for number, groups in enumerate(places)
        ],
        in_specs=[VMEM] * (1 + len(flat)),
        out_specs=[VMEM] * len(places),
        compiler_params=PARAMS,
        name="near",
    )(blocks, *flat)


def far_kernel(keep, got, high_in, low_in, out):
    incoming = jnp.concatenate(
        [keep[0, g] + got[0, g].astype(jnp.float32) for g in range(keep.shape[1])], axis=1
    )
    high, low = halves(incoming)
    rows = high.shape[0]
    both = dot(jnp.concatenate([high, low], axis=0), high_in[...])
    out[...] = both[:rows] + both[rows:] + dot(high, low_in[...])


def far(keep, got, high, low):
    return pl.pallas_call(
        far_kernel,
        out_shape=jax.ShapeDtypeStruct((keep.shape[2], high.shape[1]), jnp.float32),
        in_specs=[VMEM] * 4,
        out_specs=VMEM,
        compiler_params=PARAMS,
        name="far",
    )(keep, got, high, low)


def finish_kernel(sources, far_in, *refs):
    nears, out = refs[:-1], refs[-1]
    me = lax.axis_index("sub")
    leaf_size = nears[0].shape[2]
    pieces = [(source, nears[at][row].astype(jnp.float32)) for source, at, row in sources]
    for j in range(len(sources)):
        piece = pieces[0][1]
        for source, values in pieces[1:]:
            piece = jnp.where((me ^ source) == j, values, piece)
        columns = slice(j * leaf_size, (j + 1) * leaf_size)
        out[:, columns] = (piece + far_in[:, columns]).astype(out.dtype)


def finish(far_part, nears, sources):
    return pl.pallas_call(
        functools.partial(finish_kernel, sources),
        out_shape=jax.ShapeDtypeStruct(far_part.shape, jnp.bfloat16),
        in_specs=[VMEM] * (1 + len(nears)),
        out_specs=VMEM,
        compiler_params=PARAMS,
        name="finish",
    )(far_part, *nears)


def local(
    vectors,
    near_blocks,
    near_cols,
    near_mask,
    leaf_basis,
    transfer,
    coupling,
    far_targets,
    far_mask,
):
    leaf_count = lax.axis_size("leaf")
    sub_count = lax.axis_size("sub")
    me = lax.axis_index("leaf")
    rows = vectors.shape[0]
    steps = [bit | 1 for bit in bits_of(sub_count)]
    turn = 0
    keep, send, own = expand(vectors, leaf_basis, transfer, coupling, far_targets, far_mask)
    pair = jnp.concatenate([own, flip(vectors, "sub", steps[0])], axis=0)
    near_side = across(pair, lambda leaf: leaf ^ 1, turn)
    far_side = across(pair, lambda leaf: ((leaf + 1) ^ 1) - 1, turn)
    sides = jnp.concatenate([near_side, far_side], axis=0)
    stages = stages_of(leaf_count)
    got = flip(send, "leaf", stages[0])
    pieces = [(pair, sides)]
    for step in steps[1:]:
        pieces = pieces + [
            (flip(middle, "sub", step), flip(outer, "sub", step))
            for middle, outer in pieces
        ]
    order = span_of(steps)
    middles = [middle for middle, _ in pieces]
    outers = [outer for _, outer in pieces]
    if turn:
        outers = outers[len(outers) // 2 :] + outers[: len(outers) // 2]
    pieces = list(zip(middles, outers))
    high, low = operator(transfer, leaf_basis, keep.shape[1] * LANES)
    for bit in sorted(stages[1:], reverse=True):
        total = (keep + got.astype(keep.dtype)).reshape(2, -1, *keep.shape[1:])
        mine = (me & bit) // bit
        keep = lax.dynamic_index_in_dim(total, mine, 0, keepdims=False)
        send = lax.dynamic_index_in_dim(total, 1 - mine, 0, keepdims=False)
        got = flip(send.astype(jnp.bfloat16), "leaf", bit)
    homes = [[step ^ rest for rest in span_of(steps[n + 1 :])] for n, step in enumerate(steps)]
    places = [[order.index(0)]] + [[order.index(home) for home in group] for group in homes]
    blocks = arrange(near_blocks, near_cols, near_mask, leaf_basis.shape[0])
    made = near(pieces, blocks, rows, places)
    arrays = list(made)
    pool = {0: [(0, 0, 0)]}
    for number, group in enumerate(homes):
        for row, home in enumerate(group):
            pool[home] = [(0, number + 1, row)]
    for step, bit in enumerate(steps):
        sent = [(home, item) for home in homes[step] for item in pool[home]]
        if len(sent) == arrays[sent[0][1][1]].shape[0]:
            stack = arrays[sent[0][1][1]]
        else:
            stack = jnp.concatenate([arrays[at][row : row + 1] for _, (_, at, row) in sent], axis=0)
        arrays.append(flip(stack, "sub", bit))
        for row, (home, (source, _, _)) in enumerate(sent):
            pool[home ^ bit].append((source ^ bit, len(arrays) - 1, row))
    used = sorted({at for _, at, _ in pool[0]})
    sources = [(source, used.index(at), row) for source, at, row in pool[0]]
    far_part = far(keep, got, high, low)
    return finish(far_part, [arrays[at] for at in used], sources)


def solution(mesh):
    return jax.shard_map(
        local,
        mesh=mesh,
        in_specs=(
            P("sub", "leaf"),
            P(("leaf", "sub"), None, None, None),
            P(("leaf", "sub"), None),
            P(("leaf", "sub"), None),
            P("leaf", None, None),
            P("leaf", None, None),
            P("leaf", None, None, None),
            P("leaf", None),
            P("leaf", None),
        ),
        out_specs=P("sub", "leaf"),
        check_vma=False,
    )
```

```python
import functools

import jax
import jax.numpy as jnp
from jax import lax
from jax.experimental import pallas as pl
from jax.experimental.pallas import tpu as pltpu
from jax.sharding import PartitionSpec as P


LANES = 128
PARAMS = pltpu.CompilerParams(vmem_limit_bytes=16 * 2**20)
SMEM = pl.BlockSpec(memory_space=pltpu.SMEM)
VMEM = pl.BlockSpec(memory_space=pltpu.VMEM)
HBM = pl.BlockSpec(memory_space=pltpu.HBM)


def flip(values, axis, bit):
    count = lax.axis_size(axis)
    return lax.ppermute(values, axis, [(i, i ^ bit) for i in range(count)])


def across(values, partner, turn):
    leaf_count, sub_count = lax.axis_size("leaf"), lax.axis_size("sub")
    pairs = []
    for leaf in range(leaf_count):
        other = partner(leaf)
        inside = 0 <= other < leaf_count
        for sub in range(sub_count):
            here = leaf * sub_count + sub
            if inside:
                pairs.append((here, other * sub_count + (sub ^ turn)))
            else:
                pairs.append((here, leaf * sub_count + (sub ^ 1)))
    return lax.ppermute(values, ("leaf", "sub"), pairs)


def bits_of(count):
    bits = []
    while count > 1:
        count = count // 2
        bits.append(count)
    return bits


def stages_of(leaf_count):
    bits = bits_of(leaf_count)[::-1]
    return bits[1:] + bits[:1]


def levels_of(subtree):
    sizes = []
    while subtree >= 1:
        sizes.append(subtree)
        subtree = subtree // 2
    starts = [sum(sizes[:number]) for number in range(len(sizes))]
    return sizes, starts


def halves(values):
    high = values.astype(jnp.bfloat16)
    return high, (values - high.astype(jnp.float32)).astype(jnp.bfloat16)


def dot(left, right, contract=((1,), (0,))):
    return lax.dot_general(left, right, (contract, ((), ())), preferred_element_type=jnp.float32)


def expand_kernel(
    leaf_count, targets_in, alive_in, vectors_in, basis_in, transfer_in, coupling_in, keep, send, own, *scratch
):
    targets, alive, vectors, basis, transfer, coupling, done, *sums = scratch
    subtree, rank, leaf_size = basis.shape
    clusters, far_count = coupling.shape[:2]
    nodes = leaf_count * clusters
    sizes, starts = levels_of(subtree)
    rows = vectors.shape[0]
    bit = stages_of(leaf_count)[0]
    mine = (lax.axis_index("leaf") & bit) // bit
    copies = [
        pltpu.make_async_copy(source, target, done.at[number])
        for number, (source, target) in enumerate(
            (
                (vectors_in, vectors),
                (basis_in, basis),
                (coupling_in.at[:subtree], coupling.at[:subtree]),
                (transfer_in, transfer),
                (targets_in, targets),
                (alive_in, alive),
                (coupling_in.at[subtree:], coupling.at[subtree:]),
            )
        )
    ]
    for copy in copies:
        copy.start()
    zero = jnp.zeros((rows, rank), jnp.float32)
    shared = len(sums) < clusters
    if shared:

        def clear(row, carry):
            sums[0][row] = zero
            return carry

        lax.fori_loop(0, nodes, clear, 0)
    else:
        for number, size in enumerate(sizes):
            for c in range(starts[number], starts[number] + size):
                for tree in range(leaf_count):
                    for j in range(starts[number], starts[number] + size):
                        sums[c][tree * clusters + j] = zero
    copies[0].wait()
    own[...] = vectors[...]
    copies[1].wait()
    hats = [
        dot(vectors[:, j * leaf_size : (j + 1) * leaf_size], basis[j], ((1,), (1,)))
        for j in range(subtree)
    ]
    copies[3].wait()
    for number in range(len(sizes) - 1):
        for p in range(sizes[number + 1]):
            total = None
            for c in (starts[number] + 2 * p, starts[number] + 2 * p + 1):
                high, low = halves(hats[c])
                part = dot(high, transfer[c]) + dot(low, transfer[c])
                total = part if total is None else total + part
            hats.append(total)
    lefts = [hat.astype(jnp.bfloat16) for hat in hats]
    copies[4].wait()
    copies[5].wait()
    for wait, members in ((2, range(subtree)), (6, range(subtree, clusters))):
        copies[wait].wait()
        for k in range(far_count):
            for c in members:
                term = dot(lefts[c], coupling[c, k])
                row = jnp.where(alive[c, k] == 1, targets[c, k], nodes)
                held = sums[0 if shared else c]
                held[row] = held[row] + term
    per = LANES // rank

    def gathered(tree):
        groups = []
        for first in range(0, clusters, per):
            lanes = []
            for place in range(first, first + per):
                if place >= clusters:
                    lanes.append(zero)
                    continue
                number = max(n for n in range(len(sizes)) if starts[n] <= place)
                row = tree * clusters + place
                if shared:
                    lanes.append(sums[0][row])
                else:
                    level = range(starts[number], starts[number] + sizes[number])
                    lanes.append(sum(sums[c][row] for c in level))
            groups.append(jnp.concatenate(lanes, axis=1))
        return groups

    def emit(half, carry):
        first = (half // bit) * 2 * bit + half % bit
        for out, tree in ((keep, first + mine * bit), (send, first + (1 - mine) * bit)):
            for number, group in enumerate(gathered(tree)):
                out[half, number] = group.astype(out.dtype)
        return carry

    if leaf_count <= 8:
        for half in range(leaf_count // 2):
            emit(half, 0)
    else:
        lax.fori_loop(0, leaf_count // 2, emit, 0)


def expand(vectors, basis, transfer, coupling, targets, alive):
    leaf_count = lax.axis_size("leaf")
    clusters, _, rank = coupling.shape[:3]
    rows = vectors.shape[0]
    nodes = leaf_count * clusters
    groups = -(-clusters * rank // LANES)
    shape = (leaf_count // 2, groups, rows, LANES)
    copies = clusters if nodes <= 128 else 1
    return pl.pallas_call(
        functools.partial(expand_kernel, leaf_count),
        out_shape=[
            jax.ShapeDtypeStruct(shape, jnp.float32),
            jax.ShapeDtypeStruct(shape, jnp.bfloat16),
            jax.ShapeDtypeStruct(vectors.shape, vectors.dtype),
        ],
        in_specs=[HBM] * 6,
        out_specs=[VMEM] * 3,
        scratch_shapes=[
            pltpu.SMEM(targets.shape, targets.dtype),
            pltpu.SMEM(alive.shape, alive.dtype),
            pltpu.VMEM(vectors.shape, vectors.dtype),
            pltpu.VMEM(basis.shape, basis.dtype),
            pltpu.VMEM(transfer.shape, transfer.dtype),
            pltpu.VMEM(coupling.shape, coupling.dtype),
            pltpu.SemaphoreType.DMA((7,)),
        ]
        + [pltpu.VMEM((nodes + 1, rows, rank), jnp.float32)] * copies,
        compiler_params=PARAMS,
        name="expand",
    )(
        *(
            pltpu.with_memory_space_constraint(value, pltpu.HBM)
            for value in (targets, alive, vectors, basis, transfer, coupling)
        )
    )


def operator_kernel(transfer, basis, high_out, low_out):
    subtree, rank, leaf_size = basis.shape
    sizes, starts = levels_of(subtree)
    high_out[...] = jnp.zeros(high_out.shape, high_out.dtype)
    low_out[...] = jnp.zeros(low_out.shape, low_out.dtype)
    for j in range(subtree):
        columns = slice(j * leaf_size, (j + 1) * leaf_size)
        parts = (basis[j],)
        c = j
        for number in range(len(sizes)):
            at = slice(c * rank, (c + 1) * rank)
            high_out[at, columns] = parts[0]
            if len(parts) > 1:
                low_out[at, columns] = parts[1]
            if number + 1 < len(sizes):
                total = sum(dot(transfer[c], part, ((0,), (0,))) for part in parts)
                parts = halves(total)
                c = starts[number + 1] + (c - starts[number]) // 2


def operator(transfer, basis, depth):
    subtree, _, leaf_size = basis.shape
    shape = jax.ShapeDtypeStruct((depth, subtree * leaf_size), jnp.bfloat16)
    return pl.pallas_call(
        operator_kernel,
        out_shape=[shape, shape],
        in_specs=[VMEM, VMEM],
        out_specs=[VMEM, VMEM],
        compiler_params=PARAMS,
        name="operator",
    )(transfer, basis)


def near_kernel(*refs):
    leaves, (pair, near_side, far_side, own, away, window) = refs[:-6], refs[-6:]
    rows, points = pair.shape
    size = rows // 2
    for tree, piece in enumerate((pair, near_side, far_side)):
        window[tree] = piece[...]
    me = lax.axis_index("leaf")
    count = len(leaves) // 3
    for leaf in range(count):
        columns, alive, blocks = leaves[3 * leaf : 3 * leaf + 3]
        entries, leaf_size = blocks.shape[1:3]
        subtree = points // leaf_size
        first = me * subtree
        partner = (me ^ 1) * subtree
        total = None
        for k in range(entries):
            column = columns[0, k]
            own_tree = (column >= first) & (column < first + subtree)
            partner_tree = (column >= partner) & (column < partner + subtree)
            tree = jnp.where(own_tree, 0, jnp.where(partner_tree, 1, 2))
            start = pl.multiple_of(lax.rem(column, subtree) * leaf_size, leaf_size)
            taken = window[tree, :, pl.ds(start, leaf_size)]
            live = alive[0, k].astype(jnp.float32).astype(jnp.bfloat16)
            product = dot(taken * live, blocks[0, k])
            total = product if total is None else total + product
        own[leaf] = total[:size]
        away[leaf] = total[size:].astype(away.dtype)


def near(leaves, pair, near_side, far_side):
    rows, points = pair.shape
    leaf_size = leaves[0][2].shape[2]
    shape = (len(leaves), rows // 2, leaf_size)
    return pl.pallas_call(
        near_kernel,
        out_shape=[
            jax.ShapeDtypeStruct(shape, jnp.float32),
            jax.ShapeDtypeStruct(shape, jnp.bfloat16),
        ],
        in_specs=[SMEM, SMEM, VMEM] * len(leaves) + [VMEM] * 3,
        out_specs=[VMEM, VMEM],
        scratch_shapes=[pltpu.VMEM((3, rows, points), pair.dtype)],
        compiler_params=PARAMS,
        name="near",
    )(*[array for leaf in leaves for array in leaf], pair, near_side, far_side)


def far_kernel(keep, got, high_in, low_in, out):
    incoming = jnp.concatenate(
        [keep[0, g] + got[0, g].astype(jnp.float32) for g in range(keep.shape[1])], axis=1
    )
    high, low = halves(incoming)
    rows = high.shape[0]
    both = dot(jnp.concatenate([high, low], axis=0), high_in[...])
    out[...] = both[:rows] + both[rows:] + dot(high, low_in[...])


def far(keep, got, high, low):
    return pl.pallas_call(
        far_kernel,
        out_shape=jax.ShapeDtypeStruct((keep.shape[2], high.shape[1]), jnp.float32),
        in_specs=[VMEM] * 4,
        out_specs=VMEM,
        compiler_params=PARAMS,
        name="far",
    )(keep, got, high, low)


def finish_kernel(sources, far_in, *refs):
    nears, out = refs[:-1], refs[-1]
    me = lax.axis_index("sub")
    leaf_size = nears[0].shape[2]
    pieces = [(source, nears[at][row].astype(jnp.float32)) for source, at, row in sources]
    for j in range(len(sources)):
        piece = pieces[0][1]
        for source, values in pieces[1:]:
            piece = jnp.where((me ^ source) == j, values, piece)
        columns = slice(j * leaf_size, (j + 1) * leaf_size)
        out[:, columns] = (piece + far_in[:, columns]).astype(out.dtype)


def finish(far_part, nears, sources):
    return pl.pallas_call(
        functools.partial(finish_kernel, sources),
        out_shape=jax.ShapeDtypeStruct(far_part.shape, jnp.bfloat16),
        in_specs=[VMEM] * (1 + len(nears)),
        out_specs=VMEM,
        compiler_params=PARAMS,
        name="finish",
    )(far_part, *nears)


def local(
    vectors,
    near_blocks,
    near_cols,
    near_mask,
    leaf_basis,
    transfer,
    coupling,
    far_targets,
    far_mask,
):
    leaf_count = lax.axis_size("leaf")
    sub_count = lax.axis_size("sub")
    me = lax.axis_index("leaf")
    steps = [bit | 1 for bit in bits_of(sub_count)]
    turn = 0
    keep, send, own = expand(vectors, leaf_basis, transfer, coupling, far_targets, far_mask)
    pair = jnp.concatenate([own, flip(vectors, "sub", steps[0])], axis=0)
    near_side = across(pair, lambda leaf: leaf ^ 1, turn)
    far_side = across(pair, lambda leaf: ((leaf + 1) ^ 1) - 1, turn)
    stages = stages_of(leaf_count)
    got = flip(send, "leaf", stages[0])
    high, low = operator(transfer, leaf_basis, keep.shape[1] * LANES)
    for bit in sorted(stages[1:], reverse=True):
        total = (keep + got.astype(keep.dtype)).reshape(2, -1, *keep.shape[1:])
        mine = (me & bit) // bit
        keep = lax.dynamic_index_in_dim(total, mine, 0, keepdims=False)
        send = lax.dynamic_index_in_dim(total, 1 - mine, 0, keepdims=False)
        got = flip(send.astype(jnp.bfloat16), "leaf", bit)
    leaves = [(near_cols, near_mask, near_blocks)]
    leaves.append(
        (
            flip(near_cols, "sub", 1),
            flip(near_mask, "sub", 1),
            flip(near_blocks, "sub", 1),
        )
    )
    mine, away = near(leaves, pair, near_side, far_side)
    back = flip(away, "sub", steps[0])
    sources = [(0, 0, 0), (1, 0, 1), (steps[0], 1, 0), (steps[0] ^ 1, 1, 1)]
    far_part = far(keep, got, high, low)
    return finish(far_part, [mine, back], sources)


def solution(mesh):
    return jax.shard_map(
        local,
        mesh=mesh,
        in_specs=(
            P("sub", "leaf"),
            P(("leaf", "sub"), None, None, None),
            P(("leaf", "sub"), None),
            P(("leaf", "sub"), None),
            P("leaf", None, None),
            P("leaf", None, None),
            P("leaf", None, None, None),
            P("leaf", None),
            P("leaf", None),
        ),
        out_specs=P("sub", "leaf"),
        check_vma=False,
    )
```
